256 devices in a mesh: model: 32 (over z, y), data: 8 (over x, core).
Axes of the slice: x: 4, y: 4, z: 8, core: 2. Of those that a mesh axis runs over, the one named last changes fastest.
Arguments:
- tokens: bfloat16 [16384, 1024], P('data')
- w_up: bfloat16 [1024, 16384], P(None, 'model')
- w_down: bfloat16 [16384, 1024], P('model')
- task_heads: bfloat16 [4, 1024, 3], replicated
- labels: int32 [4, 16384], P(None, 'data')
Outputs:
- output 1: float32 [4], replicated
- output 2: float32 [1024, 16384], P('data', 'model')
- output 3: float32 [16384, 1024], P(('model', 'data'))
All inputs are finite; a program needn't handle non-finite values.
Results may differ from the reference program's by a relative error of at most 0.001.
Values are sent between devices in bfloat16 or wider.
A program may use at most 768 MiB of HBM per device.

```python
import jax
import jax.numpy as jnp
from jax import lax

HIDDEN = 1024
FFN = 16384
CLASSES = 3
TASKS = 4
TOKENS = 16384
SEGMENT = 2048
BLOCK = 256
STEPS = 20


def setup_inputs(seed: int = 0) -> dict:
    key_list = jax.random.split(jax.random.key(seed), 12)
    n_seg = TOKENS // SEGMENT
    seg_shift = jax.random.normal(key_list[0], (n_seg, 1, HIDDEN), jnp.float32)
    x_body = jax.random.normal(key_list[1], (n_seg, SEGMENT, HIDDEN), jnp.float32)
    tokens = (x_body + 0.5 * seg_shift).reshape(TOKENS, HIDDEN).astype(jnp.bfloat16)
    w_up = (jax.random.normal(key_list[2], (HIDDEN, FFN), jnp.float32) * HIDDEN ** -0.5).astype(jnp.bfloat16)
    w_down = (jax.random.normal(key_list[3], (FFN, HIDDEN), jnp.float32) * FFN ** -0.5).astype(jnp.bfloat16)
    task_sign = jnp.where(jnp.arange(TASKS) % 2 == 0, 1.0, -1.0).astype(jnp.float32)
    head_base = jax.random.normal(key_list[4], (HIDDEN, CLASSES), jnp.float32)
    head_own = jax.random.normal(key_list[5], (TASKS, HIDDEN, CLASSES), jnp.float32)
    task_heads = ((0.8 * task_sign[:, None, None] * head_base[None] + 0.6 * head_own) * (1.5 * HIDDEN ** -0.5)).astype(jnp.bfloat16)
    seg_pref = jax.random.randint(key_list[6], (n_seg, 1), 0, CLASSES)
    keep_pref = jax.random.randint(key_list[7], (n_seg, SEGMENT), 0, 4)
    any_label = jax.random.randint(key_list[8], (n_seg, SEGMENT), 0, CLASSES)
    shared = jnp.where(keep_pref < 3, seg_pref, any_label).reshape(TOKENS)
    own_label = jax.random.randint(key_list[9], (TASKS, TOKENS), 0, CLASSES)
    keep_shared = jax.random.randint(key_list[10], (TASKS, TOKENS), 0, 4)
    labels = jnp.where(keep_shared < 3, shared[None, :], own_label).astype(jnp.int32)
    return {'tokens': tokens, 'w_up': w_up, 'w_down': w_down, 'task_heads': task_heads, 'labels': labels}


def simplex_weights(gram_mat):
    trace_scale = jnp.trace(gram_mat) / TASKS

    def eg_step(weights, unused):
        updated = weights * jnp.exp(-jnp.sum(gram_mat * weights[None, :], axis=1) / trace_scale)
        return updated / jnp.sum(updated), None

    start_w = jnp.full((TASKS,), 1.0 / TASKS, jnp.float32)
    weights, unused = lax.scan(eg_step, start_w, None, length=STEPS)
    return weights


def reference(tokens, w_up, w_down, task_heads, labels):
    n_blocks = TOKENS // BLOCK
    tok_blocks = tokens.reshape(n_blocks, BLOCK, HIDDEN)
    lab_blocks = labels.reshape(TASKS, n_blocks, BLOCK).transpose(1, 0, 2)
    heads_f = task_heads.astype(jnp.float32)
    down_f = w_down.astype(jnp.float32)

    def block_grads(grad_acc, block_in):
        tok_blk, lab_blk = block_in
        pre_act = jnp.dot(tok_blk, w_up, preferred_element_type=jnp.float32)
        act_val, gelu_slope = jax.jvp(jax.nn.gelu, (pre_act,), (jnp.ones_like(pre_act),))
        act_bf = act_val.astype(jnp.bfloat16)
        mlp_out = jnp.dot(act_bf, w_down, preferred_element_type=jnp.float32)
        trunk_out = (tok_blk.astype(jnp.float32) + mlp_out).astype(jnp.bfloat16)
        logits = jnp.einsum('bd,tdc->tbc', trunk_out.astype(jnp.float32), heads_f)
        class_prob = jax.nn.softmax(logits, axis=-1)
        onehot = jax.nn.one_hot(lab_blk, CLASSES, dtype=jnp.float32)
        dlogit = (class_prob - onehot) / TOKENS
        d_trunk = jnp.einsum('tbc,tdc->tbd', dlogit, heads_f).astype(jnp.bfloat16).astype(jnp.float32)
        g_down = jnp.einsum('bf,tbd->tfd', act_bf.astype(jnp.float32), d_trunk)
        d_act = jnp.einsum('tbd,fd->tbf', d_trunk, down_f)
        d_pre = (d_act * gelu_slope[None]).astype(jnp.bfloat16).astype(jnp.float32)
        g_up = jnp.einsum('bd,tbf->tdf', tok_blk.astype(jnp.float32), d_pre)
        return (grad_acc[0] + g_up, grad_acc[1] + g_down), None

    zero_acc = (jnp.zeros((TASKS, HIDDEN, FFN), jnp.float32), jnp.zeros((TASKS, FFN, HIDDEN), jnp.float32))
    (g_up, g_down), unused = lax.scan(block_grads, zero_acc, (tok_blocks, lab_blocks))
    gram_mat = jnp.einsum('tij,sij->ts', g_up, g_up) + jnp.einsum('tij,sij->ts', g_down, g_down)
    task_weights = simplex_weights(gram_mat)
    grad_up = jnp.einsum('t,tij->ij', task_weights, g_up)
    grad_down = jnp.einsum('t,tij->ij', task_weights, g_down)
    return task_weights, grad_up, grad_down
```

```python
import functools

import jax
import jax.numpy as jnp
import numpy as np
from jax import lax
from jax.experimental import pallas as pl
from jax.experimental.pallas import tpu as pltpu
from jax.sharding import PartitionSpec as P

STEPS = 20
NY = 4
CORES = 2
F32 = jnp.float32
BF16 = jnp.bfloat16
VMEM_LIMIT = 67043328


def chain(n):
    return [(i % 2 == 0, n // 2 - (i + 1) // 2) for i in range(n - 1)]


class Ring:
    def __init__(self, n, me, peer, chunk, recv, send_sem, recv_sem, add):
        self.n, self.me, self.peer, self.chunk = n, me, peer, chunk
        self.recv, self.send_sem, self.recv_sem, self.add = recv, send_sem, recv_sem, add
        self.order = chain(n)

    def copy(self, d, i):
        far, dist = self.order[i]
        sign = 1 if d == 0 else -1
        half = d if far else 1 - d
        dest = lax.rem(self.me + self.n + sign * dist, self.n)
        target = lax.rem(self.me + self.n + sign, self.n)
        return pltpu.make_async_remote_copy(
            src_ref=self.chunk(dest, half), dst_ref=self.recv.at[d, i],
            send_sem=self.send_sem.at[d, i], recv_sem=self.recv_sem.at[d, i],
            device_id=self.peer(target), device_id_type=pl.DeviceIdType.MESH)

    def send(self, d, i):
        self.copy(d, i).start()

    def begin(self, i):
        for d in (0, 1):
            self.send(d, i)

    def step(self, i):
        for d in (0, 1):
            far, dist = self.order[i]
            sign = 1 if d == 0 else -1
            half = d if far else 1 - d
            self.copy(d, i).wait_recv()
            dest = lax.rem(self.me + self.n + sign * (dist - 1), self.n)
            self.add(dest, half, self.recv.at[d, i])
            if i + 2 <= self.n - 2:
                self.send(d, i + 2)

    def finish(self):
        for i in range(self.n - 1):
            for d in (0, 1):
                self.copy(d, i).wait_send()


def greet(peers):
    barrier = pltpu.get_barrier_semaphore()
    for peer in peers:
        pl.semaphore_signal(barrier, inc=1, device_id=peer, device_id_type=pl.DeviceIdType.MESH)
    pl.semaphore_wait(barrier, len(peers))


def forward_kernel(nz, ny, n_total, x_ref, w1_ref, w2_ref, ht_ref, lab_ref,
                   et_out, ut_hbm, sl_hbm, xt_hbm,
                   p1, p2, ut_v, sl_v, xt_v, ry1, rz1, rz2, ry2, agy, agz, zrow, logit,
                   sy1, vy1, sz1, vz1, sz2, vz2, sy2, vy2, say, vay, saz, vaz, out_sem):
    me = lax.axis_index('model')
    dat = lax.axis_index('data')
    z, y = lax.div(me, ny), lax.rem(me, ny)
    rows = p1.shape[2]
    half_rows = rows // 2
    c1, c2 = p1.shape[3], p2.shape[3]
    blk = ny * rows

    def peer_y(t):
        return (z * ny + t, dat)

    def peer_z(t):
        return (t * ny + y, dat)

    greet([peer_y(lax.rem(y + k, ny)) for k in range(1, ny)] + [peer_z(lax.rem(z + k, nz)) for k in range(1, nz)])

    def hs(half):
        return pl.ds(half * half_rows, half_rows)

    def add_y1(dest, half, buf):
        def body(k, _):
            p1[k, dest, hs(half), :] += buf[k]
            return 0
        lax.fori_loop(0, nz, body, 0)

    def add_z1(dest, half, buf):
        p1[dest, y, hs(half), :] += buf[...]

    def add_z2(dest, half, buf):
        def body(k, _):
            p2[dest, k, hs(half), :] += buf[k]
            return 0
        lax.fori_loop(0, ny, body, 0)

    def add_y2(dest, half, buf):
        p2[z, dest, hs(half), :] += buf[...]

    ring_y1 = Ring(ny, y, peer_y, lambda t, h: p1.at[:, t, hs(h), :], ry1, sy1, vy1, add_y1)
    ring_z1 = Ring(nz, z, peer_z, lambda t, h: p1.at[t, y, hs(h), :], rz1, sz1, vz1, add_z1)
    ring_z2 = Ring(nz, z, peer_z, lambda t, h: p2.at[t, :, hs(h), :], rz2, sz2, vz2, add_z2)
    ring_y2 = Ring(ny, y, peer_y, lambda t, h: p2.at[z, t, hs(h), :], ry2, sy2, vy2, add_y2)

    scale = np.float32(np.sqrt(2.0 / np.pi))

    def block(zz):
        at = pl.ds(pl.multiple_of(zz * blk, blk), blk)
        pre = jnp.dot(x_ref[at, :], w1_ref[...], preferred_element_type=F32)
        square = pre * pre
        th = jnp.tanh(scale * (pre + np.float32(0.044715) * (square * pre)))
        cdf = 0.5 * (1.0 + th)
        act = (pre * cdf).astype(BF16)
        sl_v[at, :] = cdf + 0.5 * pre * (1.0 - th * th) * (scale * (1.0 + np.float32(3 * 0.044715) * square))
        ut_v[:, at] = act.T
        part = jnp.dot(act, w2_ref[...], preferred_element_type=F32)
        p1[zz] = part[:, :c1].reshape(ny, rows, c1)
        p2[zz] = part[:, c1:].reshape(ny, rows, c2)

    far = [nz // 2]
    for k in range(nz // 2 - 1, 0, -1):
        far += [k, nz - k]
    far += [0]

    def run(first, last):
        def body(i, _):
            step = lax.div(i + 1, 2)
            off = nz // 2 + jnp.where(lax.rem(i, 2) == 1, -step, step)
            block(lax.rem(z + off, nz))
            return 0
        lax.fori_loop(first, last, body, 0)

    run(0, 1)
    ring_z2.begin(0)
    run(1, 3)
    ring_z2.begin(1)
    run(3, nz)
    ring_y1.begin(0)
    ring_y1.begin(1)

    out_copies = [pltpu.make_async_copy(ut_v, ut_hbm, out_sem.at[0]), pltpu.make_async_copy(sl_v, sl_hbm, out_sem.at[1])]
    for c in out_copies:
        c.start()

    def flip(i, _):
        at = pl.ds(pl.multiple_of(i * blk, blk), blk)
        xt_v[:, at] = x_ref[at, :].T
        return 0
    lax.fori_loop(0, nz, flip, 0)
    out_copies.append(pltpu.make_async_copy(xt_v, xt_hbm, out_sem.at[2]))
    out_copies[-1].start()

    events = [(10 + 11.3 * (i + 1), 'y1', i) for i in range(ny - 1)]
    events += [(4 + 5.6 * (i + 1), 'z2', i) for i in range(nz - 1)]
    z2_end = 4 + 5.6 * (nz - 1)
    y1_end = 10 + 11.3 * (ny - 1)
    events += [(y1_end + 0.5 + 2.2 * (i + 1), 'z1', i) for i in range(nz - 1)]
    events += [(z2_end + 1 + 3 * (i + 1), 'y2', i) for i in range(ny - 1)]
    rings = {'y1': ring_y1, 'z1': ring_z1, 'z2': ring_z2, 'y2': ring_y2}
    for _, name, i in sorted(events):
        rings[name].step(i)
        if name == 'z2' and i == nz - 2:
            ring_y2.begin(0)
            ring_y2.begin(1)
        if name == 'y1' and i == ny - 2:
            ring_z1.begin(0)
            ring_z1.begin(1)

    mine = pl.ds(pl.multiple_of(me * rows, rows), rows)
    zrow[:, :c1] = (x_ref[mine, :c1].astype(F32) + p1[z, y]).astype(BF16)
    zrow[:, c1:] = (x_ref[mine, c1:].astype(F32) + p2[z, y]).astype(BF16)
    logit[...] = lax.dot_general(ht_ref[...], zrow[...], (((1,), (1,)), ((), ())), preferred_element_type=F32)
    l0, l1, l2 = logit[0:4, :], logit[4:8, :], logit[8:12, :]
    top = jnp.maximum(jnp.maximum(l0, l1), l2)
    e0, e1, e2 = jnp.exp(l0 - top), jnp.exp(l1 - top), jnp.exp(l2 - top)
    total = e0 + e1 + e2
    wide = lab_ref[:, pl.ds(pl.multiple_of(lax.div(me, 128 // rows) * 128, 128), 128)]
    lab = wide[:, :rows]
    for k in range(1, 128 // rows):
        lab = jnp.where(lax.rem(me, 128 // rows) == k, wide[:, k * rows:(k + 1) * rows], lab)
    agy[y] = jnp.zeros((16, 128), F32)
    for c, e in enumerate((e0, e1, e2)):
        agy[y, 4 * c:4 * c + 4, 0:rows] = (e / total - jnp.where(lab == c, 1.0, 0.0)) / n_total

    def gather(n, pos, peer, buf, send_sem, recv_sem):
        sends = []
        for k in range(1, n):
            cp = pltpu.make_async_remote_copy(
                src_ref=buf.at[pos], dst_ref=buf.at[pos], send_sem=send_sem.at[k], recv_sem=recv_sem.at[k],
                device_id=peer(lax.rem(pos + k, n)), device_id_type=pl.DeviceIdType.MESH)
            cp.start()
            sends.append(cp)
        for k in range(1, n):
            src = lax.rem(pos + n - k, n)
            pltpu.make_async_remote_copy(
                src_ref=buf.at[pos], dst_ref=buf.at[src], send_sem=send_sem.at[k], recv_sem=recv_sem.at[k],
                device_id=peer(lax.rem(pos + k, n)), device_id_type=pl.DeviceIdType.MESH).wait_recv()
        return sends

    sends = gather(ny, y, peer_y, agy, say, vay)
    per = 128 // rows
    low = lax.broadcasted_iota(jnp.int32, (16, 128), 1)
    for q in range(ny // per):
        tile = agy[q * per]
        for k in range(1, per):
            tile = jnp.where(low >= k * rows, pltpu.roll(agy[q * per + k], k * rows, 1), tile)
        agz[z, :, q * 128:(q + 1) * 128] = tile
    sends += gather(nz, z, peer_z, agz, saz, vaz)
    for k in range(nz):
        et_out[:, k * blk:(k + 1) * blk] = agz[k]

    for c in sends:
        c.wait_send()
    for ring in rings.values():
        ring.finish()
    for c in out_copies:
        c.wait()


def backward_kernel(nz, ny, nx, x_shape, ut_ref, w2_ref, et_ref, h_ref, sl_hbm, xt_hbm,
                    a_out, g1_out, g2_out,
                    xt_v, sl_v, ecol, dz, da, g1, g2, d1, d2, r1, r2, gram_x, gram_y, gram_z, mat,
                    in_sem, sd, vd, sx, vx, sgx, vgx, sgy, vgy, sgz, vgz):
    me = lax.axis_index('model')
    dat = lax.axis_index('data')
    z, y = lax.div(me, ny), lax.rem(me, ny)
    x, core = lax.div(dat, CORES), lax.rem(dat, CORES)
    nd = nx * CORES
    n_tok, n_dim = x_shape
    n_ffn = ut_ref.shape[0]
    n_task = g1.shape[0]

    loads = [pltpu.make_async_copy(sl_hbm, sl_v, in_sem.at[0]), pltpu.make_async_copy(xt_hbm, xt_v, in_sem.at[1])]
    for c in loads:
        c.start()

    def peer_d(t):
        return (me, t)

    def peer_y(t):
        return (z * ny + t, dat)

    def peer_z(t):
        return (t * ny + y, dat)

    def peer_x(t):
        return (me, t * CORES + core)

    greet([peer_d(lax.rem(dat + k, nd)) for k in range(1, nd)]
          + [peer_y(lax.rem(y + k, ny)) for k in range(1, ny)]
          + [peer_z(lax.rem(z + k, nz)) for k in range(1, nz)])

    other = (me, x * CORES + 1 - core)

    def turn(i, _):
        at = pl.ds(pl.multiple_of(i * 128, 128), 128)
        ecol[at, :] = et_ref[:, at].T
        return 0
    lax.fori_loop(0, n_tok // 128, turn, 0)

    rb = 64

    def make_dz(t):
        def body(i, _):
            at = pl.ds(pl.multiple_of(i * rb, rb), rb)
            acc = ecol[at, t:t + 1] * h_ref[t:t + 1, :]
            for c in (1, 2):
                acc = acc + ecol[at, 4 * c + t:4 * c + t + 1] * h_ref[4 * c + t:4 * c + t + 1, :]
            dz[at, :] = acc.astype(BF16)
            return 0
        lax.fori_loop(0, n_tok // rb, body, 0)

    tile = 256
    q2 = g2.shape[3]
    q1 = g1.shape[3]

    def make_g2(t):
        def body(i, _):
            at = pl.ds(pl.multiple_of(i * tile, tile), tile)
            out = jnp.dot(ut_ref[...], dz[:, at], preferred_element_type=F32)
            g2[t, :, :, :, at] = out.reshape(nx, CORES, q2, tile)
            return 0
        lax.fori_loop(0, n_dim // tile, body, 0)

    def make_da():
        def body(i, _):
            at = pl.ds(pl.multiple_of(i * 2 * tile, 2 * tile), 2 * tile)
            out = lax.dot_general(dz[at, :], w2_ref[...], (((1,), (1,)), ((), ())), preferred_element_type=F32)
            da[at, :] = (out * sl_v[at, :]).astype(BF16)
            return 0
        lax.fori_loop(0, n_tok // (2 * tile), body, 0)

    def make_g1(t):
        def body(i, _):
            at = pl.ds(pl.multiple_of(i * tile, tile), tile)
            for k in (0, 1):
                hx = nx // 2
                rows = pl.ds(k * (n_dim // 2), n_dim // 2)
                out = jnp.dot(xt_v[rows, :], da[:, at], preferred_element_type=F32)
                g1[t, k * hx:(k + 1) * hx, :, :, at] = out.reshape(hx, CORES, q1, tile)
            return 0
        lax.fori_loop(0, n_ffn // tile, body, 0)

    def swap(s, g, buf):
        t = s // 2
        return pltpu.make_async_remote_copy(
            src_ref=g.at[t, :, 1 - core], dst_ref=buf.at[t], send_sem=sd.at[s], recv_sem=vd.at[s],
            device_id=other, device_id_type=pl.DeviceIdType.MESH)

    def add_swap(s, g, buf):
        t = s // 2
        swap(s, g, buf).wait_recv()

        def body(k, _):
            g[t, k, core] += buf[t, k]
            return 0
        lax.fori_loop(0, nx, body, 0)

    def ring_of(s):
        g, r, d = ((g2, r2, d2), (g1, r1, d1))[s % 2]
        t = s // 2
        half_rows = g.shape[3] // 2

        def chunk(dest, half):
            return g.at[t, dest, core, pl.ds(half * half_rows, half_rows), :]

        def add(dest, half, buf):
            g[t, dest, core, pl.ds(half * half_rows, half_rows), :] += buf[...]

        return Ring(nx, x, peer_x, chunk, r.at[t], sx.at[s], vx.at[s], add)

    n_stage = 2 * n_task
    bufs = ((g2, d2), (g1, d1))
    for s in range(n_stage):
        t = s // 2
        if s % 2 == 0:
            make_dz(t)
            make_g2(t)
        else:
            if s == 1:
                loads[0].wait()
            make_da()
            if s == 1:
                loads[1].wait()
            make_g1(t)
        swap(s, *bufs[s % 2]).start()
        if s >= 1:
            add_swap(s - 1, *bufs[(s - 1) % 2])
            ring_of(s - 1).begin(0)
            ring_of(s - 1).begin(1)
    s = n_stage - 1
    add_swap(s, *bufs[s % 2])
    ring_of(s).begin(0)
    ring_of(s).begin(1)
    for s in range(n_stage):
        ring_of(s).step(0)
    for s in range(n_stage):
        ring_of(s).step(1)
        ring_of(s).step(2)

    row_id = lax.broadcasted_iota(jnp.int32, (8, 128), 0)
    col_id = lax.broadcasted_iota(jnp.int32, (8, 128), 1)
    pairs = [(i, j) for i in range(n_task) for j in range(i, n_task)]

    def fold(g, accs):
        width = g.shape[4]

        def body(k, accs):
            at = pl.ds(pl.multiple_of(k * 8, 8), 8)
            vals = [g[t, x, core, at, :] for t in range(n_task)]
            return tuple(acc + sum((vals[i] * vals[j])[:, w:w + 128] for w in range(0, width, 128))
                         for acc, (i, j) in zip(accs, pairs))
        return lax.fori_loop(0, g.shape[3] // 8, body, accs)

    accs = tuple(jnp.zeros((8, 128), F32) for _ in pairs)
    accs = fold(g2, accs)
    accs = fold(g1, accs)
    part = jnp.zeros((8, 128), F32)
    for acc, (i, j) in zip(accs, pairs):
        hit = ((row_id == i) & (col_id == j)) | ((row_id == j) & (col_id == i))
        part = jnp.where(hit, jnp.sum(jnp.sum(acc, axis=1, keepdims=True), axis=0, keepdims=True), part)

    sends = []

    def all_sum(n, pos, peer, buf, send_sem, recv_sem, val):
        buf[pos] = val
        for k in range(1, n):
            cp = pltpu.make_async_remote_copy(
                src_ref=buf.at[pos], dst_ref=buf.at[pos], send_sem=send_sem.at[k], recv_sem=recv_sem.at[k],
                device_id=peer(lax.rem(pos + k, n)), device_id_type=pl.DeviceIdType.MESH)
            cp.start()
            sends.append(cp)
        for k in range(1, n):
            src = lax.rem(pos + n - k, n)
            pltpu.make_async_remote_copy(
                src_ref=buf.at[pos], dst_ref=buf.at[src], send_sem=send_sem.at[k], recv_sem=recv_sem.at[k],
                device_id=peer(lax.rem(pos + k, n)), device_id_type=pl.DeviceIdType.MESH).wait_recv()
        out = buf[0]
        for k in range(1, n):
            out = out + buf[k]
        return out

    part = all_sum(nd, dat, peer_d, gram_x, sgx, vgx, part)
    part = all_sum(ny, y, peer_y, gram_y, sgy, vgy, part)
    gram = all_sum(nz, z, peer_z, gram_z, sgz, vgz, part)

    eye = row_id == col_id
    live = (row_id < n_task) & (col_id < n_task)
    trace = jnp.sum(jnp.sum(jnp.where(eye & live, gram, 0.0), axis=1, keepdims=True), axis=0, keepdims=True)
    scaled = jnp.where(live, gram, 0.0)
    trace_scale = trace / n_task
    wrow = jnp.where(col_id < n_task, 1.0 / n_task, 0.0).astype(F32)
    wcol = jnp.where(row_id < n_task, 1.0 / n_task, 0.0).astype(F32)

    def eg(i, carry):
        wrow, wcol = carry
        prod = jnp.sum(scaled * wrow, axis=1, keepdims=True)
        up = wcol * jnp.exp(-prod / trace_scale)
        new = up / jnp.sum(up, axis=0, keepdims=True)
        return jnp.sum(jnp.where(eye, new, 0.0), axis=0, keepdims=True) + jnp.zeros_like(wrow), new

    wrow, wcol = lax.fori_loop(0, STEPS, eg, (wrow, wcol))
    a_out[...] = wrow
    ws = [jnp.sum(jnp.where((row_id == t) & (col_id == t), wrow, 0.0), keepdims=True)[0:1, 0:1] for t in range(n_task)]

    def mix(g, out):
        def body(k, _):
            at = pl.ds(pl.multiple_of(k * 8, 8), 8)
            acc = ws[0] * g[0, x, core, at, :]
            for t in range(1, n_task):
                acc = acc + ws[t] * g[t, x, core, at, :]
            out[at, :] = acc
            return 0
        lax.fori_loop(0, g.shape[3] // 8, body, 0)
    mix(g1, g1_out)
    mix(g2, g2_out)

    for c in sends:
        c.wait_send()
    for s in range(n_stage):
        swap(s, *bufs[s % 2]).wait_send()
        ring_of(s).finish()


def solution(mesh, ny=NY):
    n_data = mesh.shape['data']
    nz = mesh.shape['model'] // ny
    nx = n_data // CORES

    def local_step(tokens, w_up, w_down, task_heads, labels):
        n_tok, n_dim = tokens.shape
        n_ffn = w_up.shape[1]
        n_task, _, n_class = task_heads.shape
        rows = n_tok // (nz * ny)
        hr = rows // 2
        c1 = n_dim // 2
        c2 = n_dim - c1
        heads = jnp.transpose(task_heads, (2, 0, 1)).reshape(n_class * n_task, n_dim)
        heads = jnp.pad(heads, ((0, 16 - n_class * n_task), (0, 0)))
        vm = pl.BlockSpec(memory_space=pltpu.VMEM)
        hbm = pl.BlockSpec(memory_space=pl.ANY)
        dma = pltpu.SemaphoreType.DMA

        et, ut, slope, xt = pl.pallas_call(
            functools.partial(forward_kernel, nz, ny, n_tok * n_data),
            out_shape=[jax.ShapeDtypeStruct((16, n_tok), F32), jax.ShapeDtypeStruct((n_ffn, n_tok), BF16),
                       jax.ShapeDtypeStruct((n_tok, n_ffn), F32), jax.ShapeDtypeStruct((n_dim, n_tok), BF16)],
            in_specs=[vm] * 5, out_specs=[vm, hbm, hbm, hbm],
            scratch_shapes=[
                pltpu.VMEM((nz, ny, rows, c1), F32), pltpu.VMEM((nz, ny, rows, c2), F32),
                pltpu.VMEM((n_ffn, n_tok), BF16), pltpu.VMEM((n_tok, n_ffn), F32), pltpu.VMEM((n_dim, n_tok), BF16),
                pltpu.VMEM((2, ny - 1, nz, hr, c1), F32), pltpu.VMEM((2, nz - 1, hr, c1), F32),
                pltpu.VMEM((2, nz - 1, ny, hr, c2), F32), pltpu.VMEM((2, ny - 1, hr, c2), F32),
                pltpu.VMEM((ny, 16, 128), F32), pltpu.VMEM((nz, 16, ny * rows), F32),
                pltpu.VMEM((rows, n_dim), BF16), pltpu.VMEM((16, rows), F32),
                dma((2, ny - 1)), dma((2, ny - 1)), dma((2, nz - 1)), dma((2, nz - 1)),
                dma((2, nz - 1)), dma((2, nz - 1)), dma((2, ny - 1)), dma((2, ny - 1)),
                dma((ny,)), dma((ny,)), dma((nz,)), dma((nz,)), dma((3,))],
            compiler_params=pltpu.CompilerParams(collective_id=0, has_side_effects=True, vmem_limit_bytes=VMEM_LIMIT),
            name='forward',
        )(tokens, w_up, w_down, heads, labels)

        r1 = n_dim // n_data
        r2 = n_ffn // n_data
        a_tile, g1, g2 = pl.pallas_call(
            functools.partial(backward_kernel, nz, ny, nx, (n_tok, n_dim)),
            out_shape=[jax.ShapeDtypeStruct((8, 128), F32), jax.ShapeDtypeStruct((r1, n_ffn), F32),
                       jax.ShapeDtypeStruct((r2, n_dim), F32)],
            in_specs=[vm] * 4 + [hbm, hbm], out_specs=[vm, vm, vm],
            scratch_shapes=[
                pltpu.VMEM((n_dim, n_tok), BF16), pltpu.VMEM((n_tok, n_ffn), F32), pltpu.VMEM((n_tok, 16), F32),
                pltpu.VMEM((n_tok, n_dim), BF16), pltpu.VMEM((n_tok, n_ffn), BF16),
                pltpu.VMEM((n_task, nx, CORES, r1, n_ffn), F32), pltpu.VMEM((n_task, nx, CORES, r2, n_dim), F32),
                pltpu.VMEM((n_task, nx, r1, n_ffn), F32), pltpu.VMEM((n_task, nx, r2, n_dim), F32),
                pltpu.VMEM((n_task, 2, nx - 1, r1 // 2, n_ffn), F32), pltpu.VMEM((n_task, 2, nx - 1, r2 // 2, n_dim), F32),
                pltpu.VMEM((n_data, 8, 128), F32), pltpu.VMEM((ny, 8, 128), F32), pltpu.VMEM((nz, 8, 128), F32),
                pltpu.VMEM((8, 128), F32),
                dma((2,)), dma((2 * n_task,)), dma((2 * n_task,)),
                dma((2 * n_task, 2, nx - 1)), dma((2 * n_task, 2, nx - 1)),
                dma((n_data,)), dma((n_data,)), dma((ny,)), dma((ny,)), dma((nz,)), dma((nz,))],
            compiler_params=pltpu.CompilerParams(collective_id=1, has_side_effects=True, vmem_limit_bytes=VMEM_LIMIT),
            name='backward',
        )(ut, w_down, et, heads.astype(F32), slope, xt)
        return a_tile[0, :n_task], g1, g2

    return jax.shard_map(
        local_step, mesh=mesh,
        in_specs=(P('data', None), P(None, 'model'), P('model', None), P(None, None, None), P(None, 'data')),
        out_specs=(P(None), P('data', 'model'), P(('model', 'data'), None)),
        check_vma=False)
```

```python
import functools

import jax
import jax.numpy as jnp
import numpy as np
from jax import lax
from jax.experimental import pallas as pl
from jax.experimental.pallas import tpu as pltpu
from jax.sharding import PartitionSpec as P

STEPS = 20
NY = 4
CORES = 2
F32 = jnp.float32
BF16 = jnp.bfloat16
VMEM_LIMIT = 67043328


def chain(n):
    return [(i % 2 == 0, n // 2 - (i + 1) // 2) for i in range(n - 1)]


class Ring:
    def __init__(self, n, me, peer, chunk, recv, send_sem, recv_sem, add):
        self.n, self.me, self.peer, self.chunk = n, me, peer, chunk
        self.recv, self.send_sem, self.recv_sem, self.add = recv, send_sem, recv_sem, add
        self.order = chain(n)

    def copy(self, d, i):
        far, dist = self.order[i]
        sign = 1 if d == 0 else -1
        half = d if far else 1 - d
        dest = lax.rem(self.me + self.n + sign * dist, self.n)
        target = lax.rem(self.me + self.n + sign, self.n)
        return pltpu.make_async_remote_copy(
            src_ref=self.chunk(dest, half, sign * dist % self.n), dst_ref=self.recv.at[d, i],
            send_sem=self.send_sem.at[d, i], recv_sem=self.recv_sem.at[d, i],
            device_id=self.peer(target), device_id_type=pl.DeviceIdType.MESH)

    def send(self, d, i):
        self.copy(d, i).start()

    def begin(self, i):
        for d in (0, 1):
            self.send(d, i)

    def step(self, i):
        for d in (0, 1):
            far, dist = self.order[i]
            sign = 1 if d == 0 else -1
            half = d if far else 1 - d
            self.copy(d, i).wait_recv()
            dest = lax.rem(self.me + self.n + sign * (dist - 1), self.n)
            self.add(dest, half, sign * (dist - 1) % self.n, self.recv.at[d, i])
            if i + 2 <= self.n - 2:
                self.send(d, i + 2)

    def finish(self):
        for i in range(self.n - 1):
            for d in (0, 1):
                self.copy(d, i).wait_send()


def trunk_kernel(nz, ny, nx, n_total, x_hbm, w1_hbm, w2_hbm, ht_ref, lab_ref,
                 a_out, g1_out, g2_out,
                 xd, w1_v, w2_v, ht_v, hb, gg2, gg1, ut_v, sl_v, xt_v, da, ecol,
                 rya, ryb, ryc, rz1, rz2, ry2, agy, agz, zrow, logit,
                 d1, d2, r1, r2, gram_d, gram_m, m1, m2,
                 sya, vya, syb, vyb, syc, vyc, sz1, vz1, sz2, vz2, sy2, vy2, say, vay, saz, vaz,
                 w_sem, x_sem, sd, vd, sx, vx, sgd, vgd, sgm, vgm, o_sem):
    me = lax.axis_index('model')
    dat = lax.axis_index('data')
    z, y = lax.div(me, ny), lax.rem(me, ny)
    x, core = lax.div(dat, CORES), lax.rem(dat, CORES)
    n_model, nd = nz * ny, nx * CORES
    rows, n_dim = gg2.shape[2], gg2.shape[3]
    n_tok, n_ffn = sl_v.shape
    n_task = gg2.shape[0] // CORES
    half_rows = rows // 2
    c1 = rya.shape[4]
    blk = ny * rows

    def peer_y(t):
        return (z * ny + t, dat)

    def peer_z(t):
        return (t * ny + y, dat)

    def peer_m(t):
        return (t, dat)

    def peer_d(t):
        return (me, t)

    def peer_x(t):
        return (me, t * CORES + core)

    other = (me, x * CORES + 1 - core)

    def offset(i):
        step = lax.div(i + 1, 2)
        return nz // 2 + jnp.where(lax.rem(i, 2) == 1, -step, step)

    def block_rows(i):
        return pl.ds(pl.multiple_of(lax.rem(z + offset(i), nz) * blk, blk), blk)

    def load_x(i):
        at = block_rows(i)
        return pltpu.make_async_copy(x_hbm.at[at, :], xd.at[at, :], x_sem.at[i])

    load_w1 = pltpu.make_async_copy(w1_hbm, w1_v, w_sem.at[0])
    load_w2 = pltpu.make_async_copy(w2_hbm, w2_v, w_sem.at[1])
    load_w1.start()
    load_x(0).start()
    load_w2.start()

    def start_x(i, _):
        load_x(i).start()
        return 0
    lax.fori_loop(1, nz, start_x, 0)

    barrier = pltpu.get_barrier_semaphore()
    greeted = [peer_d(lax.rem(dat + k, nd)) for k in range(1, nd)]
    greeted += [peer_m(lax.rem(me + k, n_model)) for k in range(1, n_model)]
    for peer in greeted:
        pl.semaphore_signal(barrier, inc=1, device_id=peer, device_id_type=pl.DeviceIdType.MESH)

    def hs(half):
        return pl.ds(half * half_rows, half_rows)

    left, right = pl.ds(0, c1), pl.ds(c1, n_dim - c1)

    def slot(off):
        return 2 * (nz // 2 - off) - 1 if off < nz // 2 else 2 * (off - nz // 2)

    own = slot(0)

    def add_y1(first):
        def add(dest, half, off, buf):
            def body(k, _):
                gg2[first + k, dest, hs(half), left] += buf[k]
                return 0
            lax.fori_loop(0, buf.shape[0], body, 0)
        return add

    def add_z1(dest, half, off, buf):
        gg2[slot(off), y, hs(half), left] += buf[...]

    def add_z2(dest, half, off, buf):
        def body(k, _):
            gg2[slot(off), k, hs(half), right] += buf[k]
            return 0
        lax.fori_loop(0, ny, body, 0)

    def add_y2(dest, half, off, buf):
        gg2[own, dest, hs(half), right] += buf[...]

    rings = {
        'z1': Ring(nz, z, peer_z, lambda t, h, o: gg2.at[slot(o), y, hs(h), left], rz1, sz1, vz1, add_z1),
        'z2': Ring(nz, z, peer_z, lambda t, h, o: gg2.at[slot(o), :, hs(h), right], rz2, sz2, vz2, add_z2),
        'y2': Ring(ny, y, peer_y, lambda t, h, o: gg2.at[own, t, hs(h), right], ry2, sy2, vy2, add_y2),
    }
    first = 0
    for name, recv, send_sem, recv_sem in (('ya', rya, sya, vya), ('yb', ryb, syb, vyb), ('yc', ryc, syc, vyc)):
        group = pl.ds(first, recv.shape[2])
        rings[name] = Ring(ny, y, peer_y, lambda t, h, o, group=group: gg2.at[group, t, hs(h), left],
                           recv, send_sem, recv_sem, add_y1(first))
        first += recv.shape[2]

    scale = np.float32(np.sqrt(2.0 / np.pi))

    def block(i, _):
        load_x(i).wait()
        at = block_rows(i)
        pre = jnp.dot(xd[at, :], w1_v[...], preferred_element_type=F32)
        square = pre * pre
        th = jnp.tanh(scale * (pre + np.float32(0.044715) * (square * pre)))
        cdf = 0.5 * (1.0 + th)
        act = (pre * cdf).astype(BF16)
        sl_v[at, :] = cdf + 0.5 * pre * (1.0 - th * th) * (scale * (1.0 + np.float32(3 * 0.044715) * square))
        ut_v[:, at] = act.T
        part = jnp.dot(act, w2_v[...], preferred_element_type=F32)
        gg2[i] = part.reshape(ny, rows, n_dim)
        return 0

    load_w1.wait()
    load_w2.wait()
    block(0, 0)
    pl.semaphore_wait(barrier, len(greeted))
    rings['z2'].begin(0)
    lax.fori_loop(1, 3, block, 0)
    rings['ya'].begin(0)
    rings['z2'].begin(1)
    rings['ya'].begin(1)
    lax.fori_loop(3, nz, block, 0)

    def flip(i, _):
        at = pl.ds(pl.multiple_of(i * blk, blk), blk)
        xt_v[:, at] = xd[at, :].T
        return 0
    lax.fori_loop(0, nz, flip, 0)
    n_head = ht_ref.shape[0]
    ht_v[...] = jnp.zeros_like(ht_v)
    ht_v[0:n_head, :] = ht_ref[...]
    for k in range(n_head):
        hb[k] = jnp.broadcast_to(ht_v[k:k + 1, :].astype(F32), (8, n_dim))

    order = [
        ('z2', 0), ('ya', 0), ('z2', 1), ('z2', 2), ('ya', 1), ('z2', 3), ('ya', 2), ('z2', 4), ('yb', 0), ('z1', 0),
        ('yb', 1), ('z2', 5), ('yb', 2), ('z1', 1), ('z1', 2), ('z2', 6), ('yc', 0), ('yc', 1), ('y2', 0), ('y2', 1),
        ('yc', 2), ('z1', 3), ('z1', 4), ('y2', 2), ('z1', 5), ('z1', 6)]
    begins = {('ya', 0): 'yb', ('ya', 2): 'z1', ('yb', 0): 'yc', ('z2', 6): 'y2'}
    for event in order:
        name, i = event
        rings[name].step(i)
        if event in begins:
            rings[begins[event]].begin(0)
            rings[begins[event]].begin(1)

    mine = pl.ds(pl.multiple_of(me * rows, rows), rows)
    zrow[...] = (xd[mine, :].astype(F32) + gg2[own, y]).astype(BF16)
    logit[...] = lax.dot_general(ht_v[...], zrow[...], (((1,), (1,)), ((), ())), preferred_element_type=F32)
    l0, l1, l2 = logit[0:4, :], logit[4:8, :], logit[8:12, :]
    top = jnp.maximum(jnp.maximum(l0, l1), l2)
    e0, e1, e2 = jnp.exp(l0 - top), jnp.exp(l1 - top), jnp.exp(l2 - top)
    total = e0 + e1 + e2
    per = 128 // rows
    wide = lab_ref[:, pl.ds(pl.multiple_of(lax.div(me, per) * 128, 128), 128)]
    lab = wide[:, :rows]
    for k in range(1, per):
        lab = jnp.where(lax.rem(me, per) == k, wide[:, k * rows:(k + 1) * rows], lab)
    agy[y] = jnp.zeros((16, 128), F32)
    for c, e in enumerate((e0, e1, e2)):
        agy[y, 4 * c:4 * c + 4, 0:rows] = (e / total - jnp.where(lab == c, 1.0, 0.0)) / n_total

    sends = []

    def exchange(n, pos, peer, view, send_sem, recv_sem, use=None):
        def copy(k, src):
            return pltpu.make_async_remote_copy(
                src_ref=view(pos), dst_ref=view(src), send_sem=send_sem.at[k], recv_sem=recv_sem.at[k],
                device_id=peer(lax.rem(pos + k, n)), device_id_type=pl.DeviceIdType.MESH)
        for k in range(1, n):
            cp = copy(k, pos)
            cp.start()
            sends.append(cp)
        if use:
            use(pos)
        for k in range(1, n):
            src = lax.rem(pos + n - k, n)
            copy(k, src).wait_recv()
            if use:
                use(src)

    exchange(ny, y, peer_y, lambda p: agy.at[p], say, vay)
    low = lax.broadcasted_iota(jnp.int32, (16, 128), 1)
    for q in range(ny // per):
        tile = agy[q * per]
        for k in range(1, per):
            tile = jnp.where(low >= k * rows, pltpu.roll(agy[q * per + k], k * rows, 1), tile)
        agz[z, :, q * 128:(q + 1) * 128] = tile

    def turn(k):
        ecol[pl.ds(pl.multiple_of(k * blk, blk), blk), :] = agz[k].T

    exchange(nz, z, peer_z, lambda p: agz.at[p], saz, vaz, turn)
    for ring in rings.values():
        ring.finish()

    rb = 64

    def make_dz(t):
        def body(i, _):
            at = pl.ds(pl.multiple_of(i * rb, rb), rb)
            es = [jnp.broadcast_to(ecol[at, 4 * c + t:4 * c + t + 1], (rb, 128)) for c in range(3)]
            for j in range(0, n_dim, 128):
                hs3 = [jnp.concatenate([hb[4 * c + t, :, j:j + 128]] * (rb // 8), axis=0) for c in range(3)]
                xd[at, j:j + 128] = (es[0] * hs3[0] + es[1] * hs3[1] + es[2] * hs3[2]).astype(BF16)
            return 0
        lax.fori_loop(0, n_tok // rb, body, 0, unroll=4)

    tile = 256
    q1 = gg1.shape[2]

    def make_g2(t):
        def body(i, _):
            at = pl.ds(pl.multiple_of(i * tile, tile), tile)
            out = jnp.dot(ut_v[...], xd[:, at], preferred_element_type=F32).reshape(nx, CORES, rows, tile)
            for c in range(CORES):
                gg2[CORES * t + c, :, :, at] = out[:, c]
            return 0
        lax.fori_loop(0, n_dim // tile, body, 0)

    def make_da():
        def body(i, _):
            at = pl.ds(pl.multiple_of(i * 2 * tile, 2 * tile), 2 * tile)
            out = lax.dot_general(xd[at, :], w2_v[...], (((1,), (1,)), ((), ())), preferred_element_type=F32)
            da[at, :] = (out * sl_v[at, :]).astype(BF16)
            return 0
        lax.fori_loop(0, n_tok // (2 * tile), body, 0)

    def make_g1(t):
        hx = nx // 2

        def body(i, _):
            at = pl.ds(pl.multiple_of(i * tile, tile), tile)
            for k in (0, 1):
                part = pl.ds(k * (n_dim // 2), n_dim // 2)
                out = jnp.dot(xt_v[part, :], da[:, at], preferred_element_type=F32).reshape(hx, CORES, q1, tile)
                for c in range(CORES):
                    gg1[CORES * t + c, k * hx:(k + 1) * hx, :, at] = out[:, c]
            return 0
        lax.fori_loop(0, n_ffn // tile, body, 0)

    n_stage = 2 * n_task
    sets = ((gg2, d2, r2), (gg1, d1, r1))

    def swap(s):
        g, buf, _ = sets[s % 2]
        t = s // 2
        return pltpu.make_async_remote_copy(
            src_ref=g.at[CORES * t + 1 - core], dst_ref=buf.at[t], send_sem=sd.at[s], recv_sem=vd.at[s],
            device_id=other, device_id_type=pl.DeviceIdType.MESH)

    def ring_of(s):
        g, _, r = sets[s % 2]
        t = s // 2
        half = g.shape[2] // 2

        def chunk(dest, h, off):
            return g.at[CORES * t + core, dest, pl.ds(h * half, half), :]

        def add(dest, h, off, buf):
            g[CORES * t + core, dest, pl.ds(h * half, half), :] += buf[...]

        return Ring(nx, x, peer_x, chunk, r.at[t], sx.at[s], vx.at[s], add)

    def launch(s):
        g, buf, _ = sets[s % 2]
        t = s // 2
        swap(s).wait_recv()

        def body(k, _):
            g[CORES * t + core, k] += buf[t, k]
            return 0
        lax.fori_loop(0, nx, body, 0)
        if s >= 2:
            ring_of(s - 2).step(0)
        ring_of(s).begin(0)
        ring_of(s).begin(1)

    for s in range(n_stage):
        t = s // 2
        if s % 2 == 0:
            make_dz(t)
            if s >= 1:
                launch(s - 1)
            make_g2(t)
        else:
            make_da()
            launch(s - 1)
            make_g1(t)
        swap(s).start()
    launch(n_stage - 1)
    for s in (n_stage - 2, n_stage - 1):
        ring_of(s).step(0)
    for s in range(n_stage):
        ring_of(s).step(1)
        ring_of(s).step(2)

    pairs = [(i, j) for i in range(n_task) for j in range(i, n_task)]

    def fold(g, accs):
        width = g.shape[3]

        def body(k, accs):
            at = pl.ds(pl.multiple_of(k * 8, 8), 8)
            vals = [g[CORES * t + core, x, at, :] for t in range(n_task)]
            return tuple(acc + sum((vals[i] * vals[j])[:, w:w + 128] for w in range(0, width, 128))
                         for acc, (i, j) in zip(accs, pairs))
        return lax.fori_loop(0, g.shape[2] // 8, body, accs)

    accs = tuple(jnp.zeros((8, 128), F32) for _ in pairs)
    accs = fold(gg2, accs)
    accs = fold(gg1, accs)
    lane = lax.broadcasted_iota(jnp.int32, (1, 128), 1)
    part = jnp.zeros((1, 128), F32)
    for acc, (i, j) in zip(accs, pairs):
        hit = (lane == n_task * i + j) | (lane == n_task * j + i)
        part = jnp.where(hit, jnp.sum(jnp.sum(acc, axis=0, keepdims=True), axis=1, keepdims=True), part)

    def all_sum(n, pos, peer, buf, send_sem, recv_sem, val):
        buf[pos, 0:1, :] = val
        exchange(n, pos, peer, lambda p: buf.at[p, pl.ds(0, 1), :], send_sem, recv_sem)
        out = buf[0, 0:1, :]
        for k in range(1, n):
            out = out + buf[k, 0:1, :]
        return out

    part = all_sum(nd, dat, peer_d, gram_d, sgd, vgd, part)
    part = all_sum(n_model, me, peer_m, gram_m, sgm, vgm, part)

    row_id = lax.broadcasted_iota(jnp.int32, (8, 128), 0)
    col_id = lax.broadcasted_iota(jnp.int32, (8, 128), 1)
    eye = row_id == col_id
    wide8 = jnp.broadcast_to(part, (8, 128))
    gram = jnp.zeros((8, 128), F32)
    for t in range(n_task):
        moved = pltpu.roll(wide8, 128 - n_task * t, 1) if t else wide8
        gram = jnp.where((row_id == t) & (col_id < n_task), moved, gram)
    trace = jnp.sum(jnp.sum(jnp.where(eye, gram, 0.0), axis=1, keepdims=True), axis=0, keepdims=True)
    trace_scale = trace / n_task
    wrow = jnp.where(col_id < n_task, 1.0 / n_task, 0.0).astype(F32)
    wcol = jnp.where(row_id < n_task, 1.0 / n_task, 0.0).astype(F32)

    def eg(i, carry):
        wrow, wcol = carry
        prod = jnp.sum(gram * wrow, axis=1, keepdims=True)
        up = wcol * jnp.exp(-prod / trace_scale)
        new = up / jnp.sum(up, axis=0, keepdims=True)
        return jnp.sum(jnp.where(eye, new, 0.0), axis=0, keepdims=True) + jnp.zeros_like(wrow), new

    wrow, wcol = lax.fori_loop(0, STEPS, eg, (wrow, wcol))
    a_out[...] = wrow
    writes = []
    ws = [wcol[t:t + 1, :] for t in range(n_task)]

    def mix(g, out):
        width = g.shape[3]

        def body(k, _):
            at = pl.ds(pl.multiple_of(k * 8, 8), 8)
            for w in range(0, width, 128):
                acc = ws[0] * g[core, x, at, w:w + 128]
                for t in range(1, n_task):
                    acc = acc + ws[t] * g[CORES * t + core, x, at, w:w + 128]
                out[at, w:w + 128] = acc
            return 0
        lax.fori_loop(0, g.shape[2] // 8, body, 0)
    for k, (g, stage_out, out) in enumerate(((gg1, m1, g1_out), (gg2, m2, g2_out))):
        mix(g, stage_out)
        writes.append(pltpu.make_async_copy(stage_out, out, o_sem.at[k]))
        writes[-1].start()

    for c in writes:
        c.wait()
    for c in sends:
        c.wait_send()
    for s in range(n_stage):
        swap(s).wait_send()
        ring_of(s).finish()


def write_kernel(a_ref, g1_ref, g2_ref, a_out, g1_out, g2_out):
    a_out[...] = a_ref[0:1, 0:a_out.shape[1]]
    g1_out[...] = g1_ref[...]
    g2_out[...] = g2_ref[...]


def solution(mesh, ny=NY):
    n_data = mesh.shape['data']
    n_model = mesh.shape['model']
    nz = n_model // ny
    nx = n_data // CORES

    def local_step(tokens, w_up, w_down, task_heads, labels):
        n_tok, n_dim = tokens.shape
        n_ffn = w_up.shape[1]
        n_task, _, n_class = task_heads.shape
        rows = n_tok // n_model
        hr = rows // 2
        c1 = 5 * n_dim // 8
        c2 = n_dim - c1
        f1 = n_dim // n_data
        f2 = n_ffn // n_data
        heads = jnp.transpose(task_heads, (2, 0, 1)).reshape(n_class * n_task, n_dim)
        vm = pl.BlockSpec(memory_space=pltpu.VMEM)
        hbm = pl.BlockSpec(memory_space=pl.ANY)
        dma = pltpu.SemaphoreType.DMA
        outs = [jax.ShapeDtypeStruct((f1, n_ffn), F32), jax.ShapeDtypeStruct((f2, n_dim), F32)]
        stages = 2 * n_task

        results = pl.pallas_call(
            functools.partial(trunk_kernel, nz, ny, nx, n_tok * n_data),
            out_shape=[jax.ShapeDtypeStruct((8, 128), F32)] + outs,
            in_specs=[hbm] * 3 + [vm] * 2, out_specs=[vm, hbm, hbm],
            scratch_shapes=[
                pltpu.VMEM((n_tok, n_dim), BF16), pltpu.VMEM((n_dim, n_ffn), BF16), pltpu.VMEM((n_ffn, n_dim), BF16),
                pltpu.VMEM((16, n_dim), BF16), pltpu.VMEM((n_class * n_task, 8, n_dim), F32),
                pltpu.VMEM((CORES * n_task, nx, f2, n_dim), F32), pltpu.VMEM((CORES * n_task, nx, f1, n_ffn), F32),
                pltpu.VMEM((n_ffn, n_tok), BF16), pltpu.VMEM((n_tok, n_ffn), F32), pltpu.VMEM((n_dim, n_tok), BF16),
                pltpu.VMEM((n_tok, n_ffn), BF16), pltpu.VMEM((n_tok, 16), F32),
                pltpu.VMEM((2, ny - 1, 3, hr, c1), F32), pltpu.VMEM((2, ny - 1, nz - 6, hr, c1), F32),
                pltpu.VMEM((2, ny - 1, 3, hr, c1), F32), pltpu.VMEM((2, nz - 1, hr, c1), F32),
                pltpu.VMEM((2, nz - 1, ny, hr, c2), F32), pltpu.VMEM((2, ny - 1, hr, c2), F32),
                pltpu.VMEM((ny, 16, 128), F32), pltpu.VMEM((nz, 16, ny * rows), F32),
                pltpu.VMEM((rows, n_dim), BF16), pltpu.VMEM((16, rows), F32),
                pltpu.VMEM((n_task, nx, f1, n_ffn), F32), pltpu.VMEM((n_task, nx, f2, n_dim), F32),
                pltpu.VMEM((n_task, 2, nx - 1, f1 // 2, n_ffn), F32), pltpu.VMEM((n_task, 2, nx - 1, f2 // 2, n_dim), F32),
                pltpu.VMEM((n_data, 8, 128), F32), pltpu.VMEM((n_model, 8, 128), F32),
                pltpu.VMEM((f1, n_ffn), F32), pltpu.VMEM((f2, n_dim), F32),
                *[dma((2, ny - 1))] * 6, dma((2, nz - 1)), dma((2, nz - 1)),
                dma((2, nz - 1)), dma((2, nz - 1)), dma((2, ny - 1)), dma((2, ny - 1)),
                dma((ny,)), dma((ny,)), dma((nz,)), dma((nz,)),
                dma((2,)), dma((nz,)), dma((stages,)), dma((stages,)), dma((stages, 2, nx - 1)), dma((stages, 2, nx - 1)),
                dma((n_data,)), dma((n_data,)), dma((n_model,)), dma((n_model,)), dma((2,))],
            compiler_params=pltpu.CompilerParams(collective_id=0, has_side_effects=True, vmem_limit_bytes=VMEM_LIMIT),
            name='trunk',
        )(tokens, w_up, w_down, heads, labels)
        weights, g1, g2 = pl.pallas_call(
            write_kernel, out_shape=[jax.ShapeDtypeStruct((1, n_task), F32)] + outs,
            in_specs=[vm] * 3, out_specs=[vm] * 3, name='write',
        )(*results)
        return weights.reshape(n_task), g1, g2

    return jax.shard_map(
        local_step, mesh=mesh,
        in_specs=(P('data', None), P(None, 'model'), P('model', None), P(None, None, None), P(None, 'data')),
        out_specs=(P(None), P('data', 'model'), P(('model', 'data'), None)),
        check_vma=False)
```

```python
import functools

import jax
import jax.numpy as jnp
import numpy as np
from jax import lax
from jax.experimental import pallas as pl
from jax.experimental.pallas import tpu as pltpu
from jax.sharding import PartitionSpec as P

STEPS = 20
NY = 4
CORES = 2
F32 = jnp.float32
BF16 = jnp.bfloat16
VMEM_LIMIT = 67043328


def chain(n):
    return [(i % 2 == 0, n // 2 - (i + 1) // 2) for i in range(n - 1)]


class Ring:
    def __init__(self, n, me, peer, chunk, recv, send_sem, recv_sem, add):
        self.n, self.me, self.peer, self.chunk = n, me, peer, chunk
        self.recv, self.send_sem, self.recv_sem, self.add = recv, send_sem, recv_sem, add
        self.order = chain(n)

    def copy(self, d, i):
        far, dist = self.order[i]
        sign = 1 if d == 0 else -1
        half = d if far else 1 - d
        dest = lax.rem(self.me + self.n + sign * dist, self.n)
        target = lax.rem(self.me + self.n + sign, self.n)
        return pltpu.make_async_remote_copy(
            src_ref=self.chunk(dest, half, sign * dist % self.n), dst_ref=self.recv(d, i),
            send_sem=self.send_sem.at[d, i], recv_sem=self.recv_sem.at[d, i],
            device_id=self.peer(target), device_id_type=pl.DeviceIdType.MESH)

    def send(self, d, i):
        self.copy(d, i).start()

    def begin(self, i):
        for d in (0, 1):
            self.send(d, i)

    def step(self, i):
        for d in (0, 1):
            far, dist = self.order[i]
            sign = 1 if d == 0 else -1
            half = d if far else 1 - d
            self.copy(d, i).wait_recv()
            dest = lax.rem(self.me + self.n + sign * (dist - 1), self.n)
            self.add(dest, half, sign * (dist - 1) % self.n, self.recv(d, i))
            if i + 2 <= self.n - 2:
                self.send(d, i + 2)

    def finish(self):
        for i in range(self.n - 1):
            for d in (0, 1):
                self.copy(d, i).wait_send()


def trunk_kernel(nz, ny, nx, n_total, x_hbm, w1_hbm, w2_hbm, ht_ref, lab_ref,
                 a_out, g1_out, g2_out,
                 xd, w1_v, w2_v, ht_v, hb, gg2, gg1, ut_v, sl_v, xt_v, da, ecol,
                 rya, ryb, ryc, rz1, rz2, ry2, agm, zrow, logit,
                 d1, d2, r1, r2, gram_d, gram_m, m1, m2,
                 sya, vya, syb, vyb, syc, vyc, sz1, vz1, sz2, vz2, sy2, vy2, sam, vam,
                 w_sem, x_sem, sd, vd, sx, vx, sgd, vgd, sgm, vgm, o_sem):
    me = lax.axis_index('model')
    dat = lax.axis_index('data')
    z, y = lax.div(me, ny), lax.rem(me, ny)
    x, core = lax.div(dat, CORES), lax.rem(dat, CORES)
    n_model, nd = nz * ny, nx * CORES
    rows, n_dim = gg2.shape[2], gg2.shape[3]
    n_tok, n_ffn = sl_v.shape
    n_task = gg2.shape[0] // CORES
    n_class = ht_ref.shape[0]
    half_rows = rows // 2
    c1 = rya.shape[4]
    blk = ny * rows

    def peer_y(t):
        return (z * ny + t, dat)

    def peer_z(t):
        return (t * ny + y, dat)

    def peer_m(t):
        return (t, dat)

    def peer_d(t):
        return (me, t)

    def peer_x(t):
        return (me, t * CORES + core)

    other = (me, x * CORES + 1 - core)

    def offset(i):
        step = lax.div(i + 1, 2)
        return nz // 2 + jnp.where(lax.rem(i, 2) == 1, -step, step)

    def block_rows(i):
        return pl.ds(pl.multiple_of(lax.rem(z + offset(i), nz) * blk, blk), blk)

    def load_x(i):
        at = block_rows(i)
        return pltpu.make_async_copy(x_hbm.at[at, :], xd.at[at, :], x_sem.at[i])

    load_w1 = pltpu.make_async_copy(w1_hbm, w1_v, w_sem.at[0])
    load_w2 = pltpu.make_async_copy(w2_hbm, w2_v, w_sem.at[1])
    load_w1.start()
    load_x(0).start()
    load_w2.start()

    def start_x(i, _):
        load_x(i).start()
        return 0
    lax.fori_loop(1, nz, start_x, 0)

    barrier = pltpu.get_barrier_semaphore()
    greeted = [peer_d(lax.rem(dat + k, nd)) for k in range(1, nd)]
    greeted += [peer_m(lax.rem(me + k, n_model)) for k in range(1, n_model)]
    for peer in greeted:
        pl.semaphore_signal(barrier, inc=1, device_id=peer, device_id_type=pl.DeviceIdType.MESH)

    def hs(half):
        return pl.ds(half * half_rows, half_rows)

    left, right = pl.ds(0, c1), pl.ds(c1, n_dim - c1)

    def slot(off):
        return 2 * (nz // 2 - off) - 1 if off < nz // 2 else 2 * (off - nz // 2)

    own = slot(0)

    def add_y1(first):
        def add(dest, half, off, buf):
            def body(k, _):
                gg2[first + k, dest, hs(half), left] += buf[k]
                return 0
            lax.fori_loop(0, buf.shape[0], body, 0)
        return add

    def add_z1(dest, half, off, buf):
        gg2[slot(off), y, hs(half), left] += buf[...]

    def add_z2(dest, half, off, buf):
        def body(k, _):
            gg2[slot(off), k, hs(half), right] += buf[k]
            return 0
        lax.fori_loop(0, ny, body, 0)

    def add_y2(dest, half, off, buf):
        gg2[own, dest, hs(half), right] += buf[...]

    def landing(buf):
        return lambda d, i: buf.at[d, i]

    rings = {
        'z1': Ring(nz, z, peer_z, lambda t, h, o: gg2.at[slot(o), y, hs(h), left], landing(rz1), sz1, vz1, add_z1),
        'z2': Ring(nz, z, peer_z, lambda t, h, o: gg2.at[slot(o), :, hs(h), right], landing(rz2), sz2, vz2, add_z2),
        'y2': Ring(ny, y, peer_y, lambda t, h, o: gg2.at[own, t, hs(h), right], landing(ry2), sy2, vy2, add_y2),
    }
    first = 0
    for name, recv, send_sem, recv_sem in (('ya', rya, sya, vya), ('yb', ryb, syb, vyb), ('yc', ryc, syc, vyc)):
        group = pl.ds(first, recv.shape[2])
        rings[name] = Ring(ny, y, peer_y, lambda t, h, o, group=group: gg2.at[group, t, hs(h), left],
                           landing(recv), send_sem, recv_sem, add_y1(first))
        first += recv.shape[2]

    scale = np.float32(np.sqrt(2.0 / np.pi))

    def block(i, _):
        load_x(i).wait()
        at = block_rows(i)
        pre = jnp.dot(xd[at, :], w1_v[...], preferred_element_type=F32)
        square = pre * pre
        th = jnp.tanh(scale * (pre + np.float32(0.044715) * (square * pre)))
        cdf = 0.5 * (1.0 + th)
        act = (pre * cdf).astype(BF16)
        sl_v[at, :] = cdf + 0.5 * pre * (1.0 - th * th) * (scale * (1.0 + np.float32(3 * 0.044715) * square))
        ut_v[:, at] = act.T
        part = jnp.dot(act, w2_v[...], preferred_element_type=F32)
        gg2[i] = part.reshape(ny, rows, n_dim)
        return 0

    load_w1.wait()
    load_w2.wait()
    block(0, 0)
    pl.semaphore_wait(barrier, len(greeted))
    rings['z2'].begin(0)
    lax.fori_loop(1, 3, block, 0)
    rings['ya'].begin(0)
    rings['z2'].begin(1)
    rings['ya'].begin(1)
    lax.fori_loop(3, nz, block, 0)

    def flip(i, _):
        at = pl.ds(pl.multiple_of(i * blk, blk), blk)
        xt_v[:, at] = xd[at, :].T
        return 0
    lax.fori_loop(0, nz, flip, 0)
    ht_v[...] = jnp.zeros_like(ht_v)
    for c in range(n_class):
        ht_v[4 * c:4 * c + n_task, :] = ht_ref[c].astype(F32)
        for t in range(n_task):
            hb[4 * c + t] = jnp.broadcast_to(ht_ref[c, t:t + 1, :].astype(F32), (8, n_dim))

    order = [
        ('z2', 0), ('ya', 0), ('z2', 1), ('z2', 2), ('ya', 1), ('z2', 3), ('ya', 2), ('z2', 4), ('yb', 0), ('z1', 0),
        ('yb', 1), ('z2', 5), ('yb', 2), ('z1', 1), ('z1', 2), ('z2', 6), ('yc', 0), ('yc', 1), ('y2', 0), ('y2', 1),
        ('yc', 2), ('z1', 3), ('z1', 4), ('y2', 2), ('z1', 5), ('z1', 6)]
    begins = {('ya', 0): 'yb', ('ya', 2): 'z1', ('yb', 0): 'yc', ('yc', 0): 'y2'}
    for event in order:
        name, i = event
        rings[name].step(i)
        if event in begins:
            rings[begins[event]].begin(0)
            rings[begins[event]].begin(1)

    mine = pl.ds(pl.multiple_of(me * rows, rows), rows)
    zrow[...] = (xd[mine, :].astype(F32) + gg2[own, y]).astype(BF16)
    logit[...] = lax.dot_general(ht_v[...].astype(BF16), zrow[...], (((1,), (1,)), ((), ())), preferred_element_type=F32)
    per = 128 // rows
    wide = lab_ref[:, pl.ds(pl.multiple_of(lax.div(me, per) * 128, 128), 128)]
    lab = wide[:, :rows]
    for k in range(1, per):
        lab = jnp.where(lax.rem(me, per) == k, wide[:, k * rows:(k + 1) * rows], lab)
    agm[me] = jnp.zeros((8, 128), F32)
    for t in range(n_task):
        ls = [logit[4 * c + t:4 * c + t + 1, :] for c in range(n_class)]
        top = functools.reduce(jnp.maximum, ls)
        es = [jnp.exp(v - top) for v in ls]
        total = functools.reduce(jnp.add, es)
        for c in range(n_class):
            row, first = 2 * c + t // 2, t % 2 * rows
            agm[me, row:row + 1, first:first + rows] = (
                es[c] / total - jnp.where(lab[t:t + 1, :] == c, 1.0, 0.0)) / n_total

    sends = []

    def exchange(n, pos, peer, view, send_sem, recv_sem, use=None):
        def copy(k, src):
            return pltpu.make_async_remote_copy(
                src_ref=view(pos), dst_ref=view(src), send_sem=send_sem.at[k], recv_sem=recv_sem.at[k],
                device_id=peer(lax.rem(pos + k, n)), device_id_type=pl.DeviceIdType.MESH)
        for k in range(1, n):
            cp = copy(k, pos)
            cp.start()
            sends.append(cp)
        if use:
            use(pos)
        for k in range(1, n):
            src = lax.rem(pos + n - k, n)
            copy(k, src).wait_recv()
            if use:
                use(src)

    def turn(k):
        ecol[k] = agm[k].T

    exchange(n_model, me, peer_m, lambda p: agm.at[p], sam, vam, turn)
    for ring in rings.values():
        ring.finish()

    def make_dz(t, cols):
        def body(i, _):
            at = pl.ds(pl.multiple_of(i * rows, rows), rows)
            first = t % 2 * rows
            es = [jnp.broadcast_to(ecol[i, first:first + rows, 2 * c + t // 2:2 * c + t // 2 + 1], (rows, 128))
                  for c in range(n_class)]
            for j in range(cols[0], cols[1], 128):
                parts = [es[c] * jnp.concatenate([hb[4 * c + t, :, j:j + 128]] * (rows // 8), axis=0)
                         for c in range(n_class)]
                xd[at, j:j + 128] = functools.reduce(jnp.add, parts).astype(BF16)
            return 0
        lax.fori_loop(0, n_model, body, 0, unroll=4)

    tile = 256
    q1 = gg1.shape[2]

    def make_g2(t, cols):
        def body(i, _):
            at = pl.ds(pl.multiple_of(i * tile, tile), tile)
            out = jnp.dot(ut_v[...], xd[:, at], preferred_element_type=F32).reshape(nx, CORES, rows, tile)
            for c in range(CORES):
                gg2[CORES * t + c, :, :, at] = out[:, c]
            return 0
        lax.fori_loop(cols[0] // tile, cols[1] // tile, body, 0)

    def make_da():
        def body(i, _):
            at = pl.ds(pl.multiple_of(i * 2 * tile, 2 * tile), 2 * tile)
            out = lax.dot_general(xd[at, :], w2_v[...], (((1,), (1,)), ((), ())), preferred_element_type=F32)
            da[at, :] = (out * sl_v[at, :]).astype(BF16)
            return 0
        lax.fori_loop(0, n_tok // (2 * tile), body, 0)

    def make_g1(t):
        hx = nx // 2

        def body(i, _):
            at = pl.ds(pl.multiple_of(i * tile, tile), tile)
            for k in (0, 1):
                part = pl.ds(k * (n_dim // 2), n_dim // 2)
                out = jnp.dot(xt_v[part, :], da[:, at], preferred_element_type=F32).reshape(hx, CORES, q1, tile)
                for c in range(CORES):
                    gg1[CORES * t + c, k * hx:(k + 1) * hx, :, at] = out[:, c]
            return 0
        lax.fori_loop(0, n_ffn // tile, body, 0)

    all1, all2 = (0, n_ffn), (0, n_dim)
    stages = [(2, 0, (0, n_dim // 2)), (2, 0, (n_dim // 2, n_dim)), (1, 0, all1)]
    for t in range(1, n_task):
        stages += [(2, t, all2), (1, t, all1)]
    n_stage = len(stages)
    sets = {2: (gg2, d2, r2), 1: (gg1, d1, r1)}

    def columns(s):
        first, last = stages[s][2]
        return pl.ds(first, last - first)

    def swap(s):
        g, buf, _ = sets[stages[s][0]]
        t = stages[s][1]
        return pltpu.make_async_remote_copy(
            src_ref=g.at[CORES * t + 1 - core, :, :, columns(s)], dst_ref=buf.at[t, :, :, columns(s)],
            send_sem=sd.at[s], recv_sem=vd.at[s], device_id=other, device_id_type=pl.DeviceIdType.MESH)

    def ring_of(s):
        g, _, r = sets[stages[s][0]]
        t = stages[s][1]
        half = g.shape[2] // 2

        def chunk(dest, h, off):
            return g.at[CORES * t + core, dest, pl.ds(h * half, half), columns(s)]

        def add(dest, h, off, buf):
            g[CORES * t + core, dest, pl.ds(h * half, half), columns(s)] += buf[...]

        def into(d, i):
            return r.at[t, d, i, :, columns(s)]

        return Ring(nx, x, peer_x, chunk, into, sx.at[s], vx.at[s], add)

    def launch(s):
        g, buf, _ = sets[stages[s][0]]
        t = stages[s][1]
        swap(s).wait_recv()

        def body(k, _):
            g[CORES * t + core, k, :, columns(s)] += buf[t, k, :, columns(s)]
            return 0
        lax.fori_loop(0, nx, body, 0)
        if s >= 2:
            ring_of(s - 2).step(0)
        ring_of(s).begin(0)
        ring_of(s).begin(1)

    for s in range(n_stage):
        which, t, cols = stages[s]
        if which == 2:
            make_dz(t, cols)
            if s >= 2:
                launch(s - 1)
            make_g2(t, cols)
        else:
            if s == 2:
                launch(0)
            make_da()
            launch(s - 1)
            make_g1(t)
        swap(s).start()
    launch(n_stage - 1)
    for s in (n_stage - 2, n_stage - 1):
        ring_of(s).step(0)
    for s in range(n_stage):
        ring_of(s).step(1)
        ring_of(s).step(2)

    pairs = [(i, j) for i in range(n_task) for j in range(i, n_task)]

    def fold(g, accs):
        width = g.shape[3]

        def body(k, accs):
            at = pl.ds(pl.multiple_of(k * 8, 8), 8)
            vals = [g[CORES * t + core, x, at, :] for t in range(n_task)]
            return tuple(acc + sum((vals[i] * vals[j])[:, w:w + 128] for w in range(0, width, 128))
                         for acc, (i, j) in zip(accs, pairs))
        return lax.fori_loop(0, g.shape[2] // 8, body, accs)

    accs = tuple(jnp.zeros((8, 128), F32) for _ in pairs)
    accs = fold(gg2, accs)
    accs = fold(gg1, accs)
    lane = lax.broadcasted_iota(jnp.int32, (1, 128), 1)
    part = jnp.zeros((1, 128), F32)
    for acc, (i, j) in zip(accs, pairs):
        hit = (lane == n_task * i + j) | (lane == n_task * j + i)
        part = jnp.where(hit, jnp.sum(jnp.sum(acc, axis=0, keepdims=True), axis=1, keepdims=True), part)

    def all_sum(n, pos, peer, buf, send_sem, recv_sem, val):
        buf[pos, 0:1, :] = val
        exchange(n, pos, peer, lambda p: buf.at[p, pl.ds(0, 1), :], send_sem, recv_sem)
        out = buf[0, 0:1, :]
        for k in range(1, n):
            out = out + buf[k, 0:1, :]
        return out

    part = all_sum(nd, dat, peer_d, gram_d, sgd, vgd, part)
    part = all_sum(n_model, me, peer_m, gram_m, sgm, vgm, part)

    row_id = lax.broadcasted_iota(jnp.int32, (8, 128), 0)
    col_id = lax.broadcasted_iota(jnp.int32, (8, 128), 1)
    eye = row_id == col_id
    wide8 = jnp.broadcast_to(part, (8, 128))
    gram = jnp.zeros((8, 128), F32)
    for t in range(n_task):
        moved = pltpu.roll(wide8, 128 - n_task * t, 1) if t else wide8
        gram = jnp.where((row_id == t) & (col_id < n_task), moved, gram)
    trace = jnp.sum(jnp.sum(jnp.where(eye, gram, 0.0), axis=1, keepdims=True), axis=0, keepdims=True)
    trace_scale = trace / n_task
    wrow = jnp.where(col_id < n_task, 1.0 / n_task, 0.0).astype(F32)
    wcol = jnp.where(row_id < n_task, 1.0 / n_task, 0.0).astype(F32)

    def eg(i, carry):
        wrow, wcol = carry
        prod = jnp.sum(gram * wrow, axis=1, keepdims=True)
        up = wcol * jnp.exp(-prod / trace_scale)
        new = up / jnp.sum(up, axis=0, keepdims=True)
        return jnp.sum(jnp.where(eye, new, 0.0), axis=0, keepdims=True) + jnp.zeros_like(wrow), new

    wrow, wcol = lax.fori_loop(0, STEPS, eg, (wrow, wcol))
    a_out[...] = wrow
    writes = []
    ws = [wcol[t:t + 1, :] for t in range(n_task)]

    def mix(g, out):
        width = g.shape[3]

        def body(k, _):
            at = pl.ds(pl.multiple_of(k * 8, 8), 8)
            for w in range(0, width, 128):
                acc = ws[0] * g[core, x, at, w:w + 128]
                for t in range(1, n_task):
                    acc = acc + ws[t] * g[CORES * t + core, x, at, w:w + 128]
                out[at, w:w + 128] = acc
            return 0
        lax.fori_loop(0, g.shape[2] // 8, body, 0)
    for k, (g, stage_out, out) in enumerate(((gg1, m1, g1_out), (gg2, m2, g2_out))):
        mix(g, stage_out)
        writes.append(pltpu.make_async_copy(stage_out, out, o_sem.at[k]))
        writes[-1].start()

    for c in writes:
        c.wait()
    for c in sends:
        c.wait_send()
    for s in range(n_stage):
        swap(s).wait_send()
        ring_of(s).finish()


def write_kernel(a_ref, g1_ref, g2_ref, a_out, g1_out, g2_out):
    a_out[...] = a_ref[0:1, 0:a_out.shape[1]]
    g1_out[...] = g1_ref[...]
    g2_out[...] = g2_ref[...]


def solution(mesh, ny=NY):
    n_data = mesh.shape['data']
    n_model = mesh.shape['model']
    nz = n_model // ny
    nx = n_data // CORES

    def local_step(tokens, w_up, w_down, task_heads, labels):
        n_tok, n_dim = tokens.shape
        n_ffn = w_up.shape[1]
        n_task, _, n_class = task_heads.shape
        rows = n_tok // n_model
        hr = rows // 2
        c1 = 5 * n_dim // 8
        c2 = n_dim - c1
        f1 = n_dim // n_data
        f2 = n_ffn // n_data
        heads = jnp.transpose(task_heads, (2, 0, 1))
        vm = pl.BlockSpec(memory_space=pltpu.VMEM)
        hbm = pl.BlockSpec(memory_space=pl.ANY)
        dma = pltpu.SemaphoreType.DMA
        outs = [jax.ShapeDtypeStruct((f1, n_ffn), F32), jax.ShapeDtypeStruct((f2, n_dim), F32)]
        stages = 2 * n_task + 1

        results = pl.pallas_call(
            functools.partial(trunk_kernel, nz, ny, nx, n_tok * n_data),
            out_shape=[jax.ShapeDtypeStruct((8, 128), F32)] + outs,
            in_specs=[hbm] * 3 + [vm] * 2, out_specs=[vm, hbm, hbm],
            scratch_shapes=[
                pltpu.VMEM((n_tok, n_dim), BF16), pltpu.VMEM((n_dim, n_ffn), BF16), pltpu.VMEM((n_ffn, n_dim), BF16),
                pltpu.VMEM((16, n_dim), F32), pltpu.VMEM((n_class * n_task, 8, n_dim), F32),
                pltpu.VMEM((CORES * n_task, nx, f2, n_dim), F32), pltpu.VMEM((CORES * n_task, nx, f1, n_ffn), F32),
                pltpu.VMEM((n_ffn, n_tok), BF16), pltpu.VMEM((n_tok, n_ffn), F32), pltpu.VMEM((n_dim, n_tok), BF16),
                pltpu.VMEM((n_tok, n_ffn), BF16), pltpu.VMEM((n_model, 128, 8), F32),
                pltpu.VMEM((2, ny - 1, 3, hr, c1), F32), pltpu.VMEM((2, ny - 1, nz - 6, hr, c1), F32),
                pltpu.VMEM((2, ny - 1, 3, hr, c1), F32), pltpu.VMEM((2, nz - 1, hr, c1), F32),
                pltpu.VMEM((2, nz - 1, ny, hr, c2), F32), pltpu.VMEM((2, ny - 1, hr, c2), F32),
                pltpu.VMEM((n_model, 8, 128), F32),
                pltpu.VMEM((rows, n_dim), BF16), pltpu.VMEM((16, rows), F32),
                pltpu.VMEM((n_task, nx, f1, n_ffn), F32), pltpu.VMEM((n_task, nx, f2, n_dim), F32),
                pltpu.VMEM((n_task, 2, nx - 1, f1 // 2, n_ffn), F32), pltpu.VMEM((n_task, 2, nx - 1, f2 // 2, n_dim), F32),
                pltpu.VMEM((n_data, 8, 128), F32), pltpu.VMEM((n_model, 8, 128), F32),
                pltpu.VMEM((f1, n_ffn), F32), pltpu.VMEM((f2, n_dim), F32),
                *[dma((2, ny - 1))] * 6, dma((2, nz - 1)), dma((2, nz - 1)),
                dma((2, nz - 1)), dma((2, nz - 1)), dma((2, ny - 1)), dma((2, ny - 1)),
                dma((n_model,)), dma((n_model,)),
                dma((2,)), dma((nz,)), dma((stages,)), dma((stages,)), dma((stages, 2, nx - 1)), dma((stages, 2, nx - 1)),
                dma((n_data,)), dma((n_data,)), dma((n_model,)), dma((n_model,)), dma((2,))],
            compiler_params=pltpu.CompilerParams(collective_id=0, has_side_effects=True, vmem_limit_bytes=VMEM_LIMIT),
            name='trunk',
        )(tokens, w_up, w_down, heads, labels)
        weights, g1, g2 = pl.pallas_call(
            write_kernel, out_shape=[jax.ShapeDtypeStruct((1, n_task), F32)] + outs,
            in_specs=[vm] * 3, out_specs=[vm] * 3, name='write',
        )(*results)
        return weights.reshape(n_task), g1, g2

    return jax.shard_map(
        local_step, mesh=mesh,
        in_specs=(P('data', None), P(None, 'model'), P('model', None), P(None, None, None), P(None, 'data')),
        out_specs=(P(None), P('data', 'model'), P(('model', 'data'), None)),
        check_vma=False)
```

```python
import functools

import jax
import jax.numpy as jnp
import numpy as np
from jax import lax
from jax.experimental import pallas as pl
from jax.experimental.pallas import tpu as pltpu
from jax.sharding import PartitionSpec as P

STEPS = 20
NY = 4
CORES = 2
F32 = jnp.float32
BF16 = jnp.bfloat16
VMEM_LIMIT = 67043328


def chain(n):
    return [(i % 2 == 0, n // 2 - (i + 1) // 2) for i in range(n - 1)]


class Ring:
    def __init__(self, n, me, peer, chunk, recv, send_sem, recv_sem, add):
        self.n, self.me, self.peer, self.chunk = n, me, peer, chunk
        self.recv, self.send_sem, self.recv_sem, self.add = recv, send_sem, recv_sem, add
        self.order = chain(n)

    def copy(self, d, i):
        far, dist = self.order[i]
        sign = 1 if d == 0 else -1
        half = d if far else 1 - d
        dest = lax.rem(self.me + self.n + sign * dist, self.n)
        target = lax.rem(self.me + self.n + sign, self.n)
        return pltpu.make_async_remote_copy(
            src_ref=self.chunk(dest, half, sign * dist % self.n), dst_ref=self.recv(d, i),
            send_sem=self.send_sem, recv_sem=self.recv_sem.at[d, i],
            device_id=self.peer(target), device_id_type=pl.DeviceIdType.MESH)

    def send(self, d, i):
        self.copy(d, i).start()

    def begin(self, i):
        for d in (0, 1):
            self.send(d, i)

    def step(self, i):
        for d in (0, 1):
            far, dist = self.order[i]
            sign = 1 if d == 0 else -1
            half = d if far else 1 - d
            self.copy(d, i).wait_recv()
            dest = lax.rem(self.me + self.n + sign * (dist - 1), self.n)
            self.add(dest, half, sign * (dist - 1) % self.n, self.recv(d, i))
            if i + 2 <= self.n - 2:
                self.send(d, i + 2)


def sent(buf, send_sem, recv_sem, peer):
    pltpu.make_async_remote_copy(
        src_ref=buf, dst_ref=buf, send_sem=send_sem, recv_sem=recv_sem,
        device_id=peer, device_id_type=pl.DeviceIdType.MESH).wait_send()


def trunk_kernel(nz, ny, nx, n_total, x_hbm, w1_hbm, w2_hbm, ht_ref, lab_ref,
                 a_out, g1_out, g2_out,
                 xd, w1_v, w2_v, ht_v, hb, gg2, gg1, ut_v, sl_v, xt_v, da, ecol,
                 rya, ryb, ryc, rz1, rz2, ry2, agm, zrow, logit,
                 d1, d2, r1, r2, gram_d, gram_m, m1, m2,
                 sya, vya, syb, vyb, syc, vyc, sz1, vz1, sz2, vz2, sy2, vy2, sam, vam,
                 w_sem, x_sem, sd, vd, sx, vx, sgd, vgd, sgm, vgm, o_sem):
    me = lax.axis_index('model')
    dat = lax.axis_index('data')
    z, y = lax.div(me, ny), lax.rem(me, ny)
    x, core = lax.div(dat, CORES), lax.rem(dat, CORES)
    n_model, nd = nz * ny, nx * CORES
    rows, n_dim = gg2.shape[2], gg2.shape[3]
    n_tok, n_ffn = sl_v.shape
    n_task = gg2.shape[0] // CORES
    n_class = ht_ref.shape[0]
    half_rows = rows // 2
    c1 = rya.shape[4]
    blk = ny * rows

    def peer_y(t):
        return (z * ny + t, dat)

    def peer_z(t):
        return (t * ny + y, dat)

    def peer_m(t):
        return (t, dat)

    def peer_d(t):
        return (me, t)

    def peer_x(t):
        return (me, t * CORES + core)

    other = (me, x * CORES + 1 - core)

    def offset(i):
        step = lax.div(i + 1, 2)
        return nz // 2 + jnp.where(lax.rem(i, 2) == 1, -step, step)

    def block_rows(i):
        return pl.ds(pl.multiple_of(lax.rem(z + offset(i), nz) * blk, blk), blk)

    def load_x(i):
        at = block_rows(i)
        return pltpu.make_async_copy(x_hbm.at[at, :], xd.at[at, :], x_sem.at[i])

    load_w1 = pltpu.make_async_copy(w1_hbm, w1_v, w_sem.at[0])
    load_w2 = pltpu.make_async_copy(w2_hbm, w2_v, w_sem.at[1])
    load_w1.start()
    load_x(0).start()
    load_w2.start()

    def start_x(i, _):
        load_x(i).start()
        return 0
    lax.fori_loop(1, nz, start_x, 0)

    barrier = pltpu.get_barrier_semaphore()
    greeted = [peer_d(lax.rem(dat + k, nd)) for k in range(1, nd)]
    greeted += [peer_m(lax.rem(me + k, n_model)) for k in range(1, n_model)]
    for peer in greeted:
        pl.semaphore_signal(barrier, inc=1, device_id=peer, device_id_type=pl.DeviceIdType.MESH)

    def hs(half):
        return pl.ds(half * half_rows, half_rows)

    left, right = pl.ds(0, c1), pl.ds(c1, n_dim - c1)

    def slot(off):
        return 2 * (nz // 2 - off) - 1 if off < nz // 2 else 2 * (off - nz // 2)

    own = slot(0)

    def add_y1(first):
        def add(dest, half, off, buf):
            def body(k, _):
                gg2[first + k, dest, hs(half), left] += buf[k]
                return 0
            lax.fori_loop(0, buf.shape[0], body, 0)
        return add

    def add_z1(dest, half, off, buf):
        gg2[slot(off), y, hs(half), left] += buf[...]

    def add_z2(dest, half, off, buf):
        def body(k, _):
            gg2[slot(off), k, hs(half), right] += buf[k]
            return 0
        lax.fori_loop(0, ny, body, 0)

    def add_y2(dest, half, off, buf):
        gg2[own, dest, hs(half), right] += buf[...]

    def landing(buf):
        return lambda d, i: buf.at[d, i]

    rings = {
        'z1': Ring(nz, z, peer_z, lambda t, h, o: gg2.at[slot(o), y, hs(h), left], landing(rz1), sz1.at[0], vz1, add_z1),
        'z2': Ring(nz, z, peer_z, lambda t, h, o: gg2.at[slot(o), :, hs(h), right], landing(rz2), sz2.at[0], vz2, add_z2),
        'y2': Ring(ny, y, peer_y, lambda t, h, o: gg2.at[own, t, hs(h), right], landing(ry2), sy2.at[0], vy2, add_y2),
    }
    first = 0
    for name, recv, send_sem, recv_sem in (('ya', rya, sya, vya), ('yb', ryb, syb, vyb), ('yc', ryc, syc, vyc)):
        group = pl.ds(first, recv.shape[2])
        rings[name] = Ring(ny, y, peer_y, lambda t, h, o, group=group: gg2.at[group, t, hs(h), left],
                           landing(recv), send_sem.at[0], recv_sem, add_y1(first))
        first += recv.shape[2]

    scale = np.float32(np.sqrt(2.0 / np.pi))

    def block(i, _):
        load_x(i).wait()
        at = block_rows(i)
        pre = jnp.dot(xd[at, :], w1_v[...], preferred_element_type=F32)
        square = pre * pre
        th = jnp.tanh(scale * (pre + np.float32(0.044715) * (square * pre)))
        cdf = 0.5 * (1.0 + th)
        act = (pre * cdf).astype(BF16)
        sl_v[at, :] = cdf + 0.5 * pre * (1.0 - th * th) * (scale * (1.0 + np.float32(3 * 0.044715) * square))
        ut_v[:, at] = act.T
        part = jnp.dot(act, w2_v[...], preferred_element_type=F32)
        gg2[i] = part.reshape(ny, rows, n_dim)
        return 0

    load_w1.wait()
    load_w2.wait()
    block(0, 0)
    pl.semaphore_wait(barrier, len(greeted))
    rings['z2'].begin(0)
    lax.fori_loop(1, 3, block, 0)
    rings['ya'].begin(0)
    rings['z2'].begin(1)
    rings['ya'].begin(1)
    lax.fori_loop(3, nz, block, 0)

    def flip(i, _):
        at = pl.ds(pl.multiple_of(i * blk, blk), blk)
        xt_v[:, at] = xd[at, :].T
        return 0
    lax.fori_loop(0, nz, flip, 0)
    ht_v[...] = jnp.zeros_like(ht_v)
    for c in range(n_class):
        ht_v[4 * c:4 * c + n_task, :] = ht_ref[c].astype(F32)
        for t in range(n_task):
            hb[4 * c + t] = jnp.broadcast_to(ht_ref[c, t:t + 1, :].astype(F32), (8, n_dim))

    order = [
        ('z2', 0), ('ya', 0), ('z2', 1), ('z2', 2), ('ya', 1), ('z2', 3), ('ya', 2), ('z2', 4), ('yb', 0), ('z1', 0),
        ('yb', 1), ('z2', 5), ('yb', 2), ('z1', 1), ('z1', 2), ('z2', 6), ('yc', 0), ('yc', 1), ('yc', 2), ('z1', 3),
        ('z1', 4), ('y2', 0), ('y2', 1), ('z1', 5), ('y2', 2), ('z1', 6)]
    begins = {('ya', 0): 'yb', ('ya', 2): 'z1', ('yb', 0): 'yc', ('yc', 0): 'y2'}
    for event in order:
        name, i = event
        rings[name].step(i)
        if event in begins:
            rings[begins[event]].begin(0)
            rings[begins[event]].begin(1)

    mine = pl.ds(pl.multiple_of(me * rows, rows), rows)
    zrow[...] = (xd[mine, :].astype(F32) + gg2[own, y]).astype(BF16)
    logit[...] = lax.dot_general(ht_v[...].astype(BF16), zrow[...], (((1,), (1,)), ((), ())), preferred_element_type=F32)
    per = 128 // rows
    wide = lab_ref[:, pl.ds(pl.multiple_of(lax.div(me, per) * 128, 128), 128)]
    lab = wide[:, :rows]
    for k in range(1, per):
        lab = jnp.where(lax.rem(me, per) == k, wide[:, k * rows:(k + 1) * rows], lab)
    agm[me] = jnp.zeros((8, 128), F32)
    for t in range(n_task):
        ls = [logit[4 * c + t:4 * c + t + 1, :] for c in range(n_class)]
        top = functools.reduce(jnp.maximum, ls)
        es = [jnp.exp(v - top) for v in ls]
        total = functools.reduce(jnp.add, es)
        for c in range(n_class):
            row, first = 2 * c + t // 2, t % 2 * rows
            agm[me, row:row + 1, first:first + rows] = (
                es[c] / total - jnp.where(lab[t:t + 1, :] == c, 1.0, 0.0)) / n_total

    def exchange(n, pos, peer, buf, send_sem, recv_sem, use):
        def copy(k, src):
            return pltpu.make_async_remote_copy(
                src_ref=buf.at[pos], dst_ref=buf.at[src], send_sem=send_sem.at[0], recv_sem=recv_sem.at[k],
                device_id=peer(lax.rem(pos + k, n)), device_id_type=pl.DeviceIdType.MESH)
        for k in range(1, n):
            copy(k, pos).start()
        use(pos)
        for k in range(1, n):
            src = lax.rem(pos + n - k, n)
            copy(k, src).wait_recv()
            use(src)

    def turn(k):
        ecol[k] = agm[k].T

    exchange(n_model, me, peer_m, agm, sam, vam, turn)
    for buf, send_sem, recv_sem in ((rya, sya, vya), (ryb, syb, vyb), (ryc, syc, vyc), (rz1, sz1, vz1), (rz2, sz2, vz2),
                                    (ry2, sy2, vy2)):
        sent(buf, send_sem.at[0], recv_sem.at[0, 0], other)

    def make_dz(t, cols):
        def body(i, _):
            at = pl.ds(pl.multiple_of(i * rows, rows), rows)
            first = t % 2 * rows
            es = [jnp.broadcast_to(ecol[i, first:first + rows, 2 * c + t // 2:2 * c + t // 2 + 1], (rows, 128))
                  for c in range(n_class)]
            for j in range(cols[0], cols[1], 128):
                parts = [es[c] * jnp.concatenate([hb[4 * c + t, :, j:j + 128]] * (rows // 8), axis=0)
                         for c in range(n_class)]
                xd[at, j:j + 128] = functools.reduce(jnp.add, parts).astype(BF16)
            return 0
        lax.fori_loop(0, n_model, body, 0, unroll=4)

    tile = 256
    q1 = gg1.shape[2]

    def make_g2(t, cols):
        def body(i, _):
            at = pl.ds(pl.multiple_of(i * tile, tile), tile)
            out = jnp.dot(ut_v[...], xd[:, at], preferred_element_type=F32).reshape(nx, CORES, rows, tile)
            for c in range(CORES):
                gg2[CORES * t + c, :, :, at] = out[:, c]
            return 0
        lax.fori_loop(cols[0] // tile, cols[1] // tile, body, 0)

    def make_da():
        def body(i, _):
            at = pl.ds(pl.multiple_of(i * 2 * tile, 2 * tile), 2 * tile)
            out = lax.dot_general(xd[at, :], w2_v[...], (((1,), (1,)), ((), ())), preferred_element_type=F32)
            da[at, :] = (out * sl_v[at, :]).astype(BF16)
            return 0
        lax.fori_loop(0, n_tok // (2 * tile), body, 0)

    def make_g1(t):
        hx = nx // 2

        def body(i, _):
            at = pl.ds(pl.multiple_of(i * tile, tile), tile)
            for k in (0, 1):
                part = pl.ds(k * (n_dim // 2), n_dim // 2)
                out = jnp.dot(xt_v[part, :], da[:, at], preferred_element_type=F32).reshape(hx, CORES, q1, tile)
                for c in range(CORES):
                    gg1[CORES * t + c, k * hx:(k + 1) * hx, :, at] = out[:, c]
            return 0
        lax.fori_loop(0, n_ffn // tile, body, 0)

    all1, all2 = (0, n_ffn), (0, n_dim)
    stages = [(2, 0, (0, n_dim // 2)), (2, 0, (n_dim // 2, n_dim)), (1, 0, all1)]
    for t in range(1, n_task):
        stages += [(2, t, all2), (1, t, all1)]
    n_stage = len(stages)
    sets = {2: (gg2, d2, r2), 1: (gg1, d1, r1)}

    def columns(s):
        first, last = stages[s][2]
        return pl.ds(first, last - first)

    def swap(s):
        g, buf, _ = sets[stages[s][0]]
        t = stages[s][1]
        return pltpu.make_async_remote_copy(
            src_ref=g.at[CORES * t + 1 - core, :, :, columns(s)], dst_ref=buf.at[t, :, :, columns(s)],
            send_sem=sd.at[stages[s][0] - 1], recv_sem=vd.at[s], device_id=other, device_id_type=pl.DeviceIdType.MESH)

    def ring_of(s):
        g, _, r = sets[stages[s][0]]
        t = stages[s][1]
        half = g.shape[2] // 2

        def chunk(dest, h, off):
            return g.at[CORES * t + core, dest, pl.ds(h * half, half), columns(s)]

        def add(dest, h, off, buf):
            g[CORES * t + core, dest, pl.ds(h * half, half), columns(s)] += buf[...]

        def into(d, i):
            return r.at[t, d, i, :, columns(s)]

        return Ring(nx, x, peer_x, chunk, into, sx.at[stages[s][0] - 1], vx.at[s], add)

    def launch(s):
        g, buf, _ = sets[stages[s][0]]
        t = stages[s][1]
        swap(s).wait_recv()

        def body(k, _):
            g[CORES * t + core, k, :, columns(s)] += buf[t, k, :, columns(s)]
            return 0
        lax.fori_loop(0, nx, body, 0)
        if s == 2:
            ring_of(1).step(0)
        if s >= 4:
            ring_of(s - 2).step(0)
        ring_of(s).begin(0)
        ring_of(s).begin(1)

    for s in range(n_stage):
        which, t, cols = stages[s]
        if which == 2:
            make_dz(t, cols)
            if s >= 2:
                launch(s - 1)
            make_g2(t, cols)
        else:
            if s == 2:
                launch(0)
            make_da()
            launch(s - 1)
            make_g1(t)
            if s == 2:
                ring_of(0).step(0)
        swap(s).start()
    launch(n_stage - 1)
    for s in (n_stage - 2, n_stage - 1):
        ring_of(s).step(0)
    for s in range(n_stage):
        ring_of(s).step(1)
        ring_of(s).step(2)

    pairs = [(i, j) for i in range(n_task) for j in range(i, n_task)]

    def fold(g, accs):
        width = g.shape[3]

        def body(k, accs):
            at = pl.ds(pl.multiple_of(k * 8, 8), 8)
            vals = [g[CORES * t + core, x, at, :] for t in range(n_task)]
            return tuple(acc + sum((vals[i] * vals[j])[:, w:w + 128] for w in range(0, width, 128))
                         for acc, (i, j) in zip(accs, pairs))
        return lax.fori_loop(0, g.shape[2] // 8, body, accs)

    accs = tuple(jnp.zeros((8, 128), F32) for _ in pairs)
    accs = fold(gg2, accs)
    accs = fold(gg1, accs)
    lane = lax.broadcasted_iota(jnp.int32, (1, 128), 1)
    part = jnp.zeros((1, 128), F32)
    for acc, (i, j) in zip(accs, pairs):
        hit = (lane == n_task * i + j) | (lane == n_task * j + i)
        part = jnp.where(hit, jnp.sum(jnp.sum(acc, axis=0, keepdims=True), axis=1, keepdims=True), part)

    def all_sum(n, pos, peer, buf, send_sem, recv_sem, val):
        buf[pos, 0:1, :] = val
        for k in range(1, n):
            pltpu.make_async_remote_copy(
                src_ref=buf.at[pos, pl.ds(0, 1), :], dst_ref=buf.at[pos, pl.ds(0, 1), :],
                send_sem=send_sem.at[0], recv_sem=recv_sem.at[k],
                device_id=peer(lax.rem(pos + k, n)), device_id_type=pl.DeviceIdType.MESH).start()
        for k in range(1, n):
            src = lax.rem(pos + n - k, n)
            pltpu.make_async_remote_copy(
                src_ref=buf.at[src, pl.ds(0, 1), :], dst_ref=buf.at[src, pl.ds(0, 1), :],
                send_sem=send_sem.at[0], recv_sem=recv_sem.at[k],
                device_id=peer(src), device_id_type=pl.DeviceIdType.MESH).wait_recv()
        out = buf[0, 0:1, :]
        for k in range(1, n):
            out = out + buf[k, 0:1, :]
        return out

    part = all_sum(nd, dat, peer_d, gram_d, sgd, vgd, part)
    part = all_sum(n_model, me, peer_m, gram_m, sgm, vgm, part)

    gram = [[jnp.broadcast_to(part[:, n_task * i + j:n_task * i + j + 1], (1, 128)) for j in range(n_task)]
            for i in range(n_task)]
    trace_scale = functools.reduce(jnp.add, [gram[i][i] for i in range(n_task)]) / n_task

    def eg(i, ws):
        ups = []
        for t in range(n_task):
            prod = functools.reduce(jnp.add, [gram[t][j] * ws[j] for j in range(n_task)])
            ups.append(ws[t] * jnp.exp(-prod / trace_scale))
        total = functools.reduce(jnp.add, ups)
        return tuple(up / total for up in ups)

    ws = tuple(jnp.full((1, 128), 1.0 / n_task, F32) for _ in range(n_task))
    ws = lax.fori_loop(0, STEPS, eg, ws)
    weights = jnp.zeros((1, 128), F32)
    for t in range(n_task):
        weights = jnp.where(lane == t, ws[t], weights)
    a_out[0:1, :] = weights
    writes = []

    def mix(g, out):
        width = g.shape[3]

        def body(k, _):
            at = pl.ds(pl.multiple_of(k * 8, 8), 8)
            for w in range(0, width, 128):
                acc = ws[0] * g[core, x, at, w:w + 128]
                for t in range(1, n_task):
                    acc = acc + ws[t] * g[CORES * t + core, x, at, w:w + 128]
                out[at, w:w + 128] = acc
            return 0
        lax.fori_loop(0, g.shape[2] // 8, body, 0)
    for k, (g, stage_out, out) in enumerate(((gg1, m1, g1_out), (gg2, m2, g2_out))):
        mix(g, stage_out)
        writes.append(pltpu.make_async_copy(stage_out, out, o_sem.at[k]))
        writes[-1].start()

    for c in writes:
        c.wait()
    sent(agm.at[pl.ds(0, n_model - 1)], sam.at[0], vam.at[0], other)
    sent(gram_d.at[pl.ds(0, nd - 1), pl.ds(0, 1), :], sgd.at[0], vgd.at[0], other)
    sent(gram_m.at[pl.ds(0, n_model - 1), pl.ds(0, 1), :], sgm.at[0], vgm.at[0], other)
    for k, (d, r) in enumerate(((d1, r1), (d2, r2))):
        sent(d, sd.at[k], vd.at[0], other)
        sent(r, sx.at[k], vx.at[0, 0, 0], other)


def write_kernel(a_ref, g1_ref, g2_ref, a_out, g1_out, g2_out):
    a_out[...] = a_ref[0:1, 0:a_out.shape[1]]
    g1_out[...] = g1_ref[...]
    g2_out[...] = g2_ref[...]


def solution(mesh, ny=NY):
    n_data = mesh.shape['data']
    n_model = mesh.shape['model']
    nz = n_model // ny
    nx = n_data // CORES

    def local_step(tokens, w_up, w_down, task_heads, labels):
        n_tok, n_dim = tokens.shape
        n_ffn = w_up.shape[1]
        n_task, _, n_class = task_heads.shape
        rows = n_tok // n_model
        hr = rows // 2
        c1 = 5 * n_dim // 8
        c2 = n_dim - c1
        f1 = n_dim // n_data
        f2 = n_ffn // n_data
        heads = jnp.transpose(task_heads, (2, 0, 1))
        vm = pl.BlockSpec(memory_space=pltpu.VMEM)
        hbm = pl.BlockSpec(memory_space=pl.ANY)
        dma = pltpu.SemaphoreType.DMA
        outs = [jax.ShapeDtypeStruct((f1, n_ffn), F32), jax.ShapeDtypeStruct((f2, n_dim), F32)]
        stages = 2 * n_task + 1

        results = pl.pallas_call(
            functools.partial(trunk_kernel, nz, ny, nx, n_tok * n_data),
            out_shape=[jax.ShapeDtypeStruct((8, 128), F32)] + outs,
            in_specs=[hbm] * 3 + [vm] * 2, out_specs=[vm, hbm, hbm],
            scratch_shapes=[
                pltpu.VMEM((n_tok, n_dim), BF16), pltpu.VMEM((n_dim, n_ffn), BF16), pltpu.VMEM((n_ffn, n_dim), BF16),
                pltpu.VMEM((16, n_dim), F32), pltpu.VMEM((n_class * n_task, 8, n_dim), F32),
                pltpu.VMEM((CORES * n_task, nx, f2, n_dim), F32), pltpu.VMEM((CORES * n_task, nx, f1, n_ffn), F32),
                pltpu.VMEM((n_ffn, n_tok), BF16), pltpu.VMEM((n_tok, n_ffn), F32), pltpu.VMEM((n_dim, n_tok), BF16),
                pltpu.VMEM((n_tok, n_ffn), BF16), pltpu.VMEM((n_model, 128, 8), F32),
                pltpu.VMEM((2, ny - 1, 3, hr, c1), F32), pltpu.VMEM((2, ny - 1, nz - 6, hr, c1), F32),
                pltpu.VMEM((2, ny - 1, 3, hr, c1), F32), pltpu.VMEM((2, nz - 1, hr, c1), F32),
                pltpu.VMEM((2, nz - 1, ny, hr, c2), F32), pltpu.VMEM((2, ny - 1, hr, c2), F32),
                pltpu.VMEM((n_model, 8, 128), F32),
                pltpu.VMEM((rows, n_dim), BF16), pltpu.VMEM((16, rows), F32),
                pltpu.VMEM((n_task, nx, f1, n_ffn), F32), pltpu.VMEM((n_task, nx, f2, n_dim), F32),
                pltpu.VMEM((n_task, 2, nx - 1, f1 // 2, n_ffn), F32), pltpu.VMEM((n_task, 2, nx - 1, f2 // 2, n_dim), F32),
                pltpu.VMEM((n_data, 8, 128), F32), pltpu.VMEM((n_model, 8, 128), F32),
                pltpu.VMEM((f1, n_ffn), F32), pltpu.VMEM((f2, n_dim), F32),
                *[dma((1,)), dma((2, ny - 1))] * 3, dma((1,)), dma((2, nz - 1)),
                dma((1,)), dma((2, nz - 1)), dma((1,)), dma((2, ny - 1)),
                dma((1,)), dma((n_model,)),
                dma((2,)), dma((nz,)), dma((2,)), dma((stages,)), dma((2,)), dma((stages, 2, nx - 1)),
                dma((1,)), dma((n_data,)), dma((1,)), dma((n_model,)), dma((2,))],
            compiler_params=pltpu.CompilerParams(collective_id=0, has_side_effects=True, vmem_limit_bytes=VMEM_LIMIT),
            name='trunk',
        )(tokens, w_up, w_down, heads, labels)
        weights, g1, g2 = pl.pallas_call(
            write_kernel, out_shape=[jax.ShapeDtypeStruct((1, n_task), F32)] + outs,
            in_specs=[vm] * 3, out_specs=[vm] * 3, name='write',
        )(*results)
        return weights.reshape(n_task), g1, g2

    return jax.shard_map(
        local_step, mesh=mesh,
        in_specs=(P('data', None), P(None, 'model'), P('model', None), P(None, None, None), P(None, 'data')),
        out_specs=(P(None), P('data', 'model'), P(('model', 'data'), None)),
        check_vma=False)
```

```python
import functools

import jax
import jax.numpy as jnp
import numpy as np
from jax import lax
from jax.experimental import pallas as pl
from jax.experimental.pallas import tpu as pltpu
from jax.sharding import PartitionSpec as P

STEPS = 20
NY = 4
CORES = 2
F32 = jnp.float32
BF16 = jnp.bfloat16
VMEM_LIMIT = 67043328


def chain(n):
    return [(i % 2 == 0, n // 2 - (i + 1) // 2) for i in range(n - 1)]


class Ring:
    def __init__(self, n, me, peer, chunk, recv, send_sem, recv_sem, add):
        self.n, self.me, self.peer, self.chunk = n, me, peer, chunk
        self.recv, self.send_sem, self.recv_sem, self.add = recv, send_sem, recv_sem, add
        self.order = chain(n)

    def copy(self, d, i):
        far, dist = self.order[i]
        sign = 1 if d == 0 else -1
        half = d if far else 1 - d
        dest = lax.rem(self.me + self.n + sign * dist, self.n)
        target = lax.rem(self.me + self.n + sign, self.n)
        return pltpu.make_async_remote_copy(
            src_ref=self.chunk(dest, half, sign * dist % self.n), dst_ref=self.recv(d, i),
            send_sem=self.send_sem, recv_sem=self.recv_sem.at[d, i],
            device_id=self.peer(target), device_id_type=pl.DeviceIdType.MESH)

    def send(self, d, i):
        self.copy(d, i).start()

    def begin(self, i):
        for d in (0, 1):
            self.send(d, i)

    def step(self, i):
        for d in (0, 1):
            far, dist = self.order[i]
            sign = 1 if d == 0 else -1
            half = d if far else 1 - d
            self.copy(d, i).wait_recv()
            dest = lax.rem(self.me + self.n + sign * (dist - 1), self.n)
            self.add(dest, half, sign * (dist - 1) % self.n, self.recv(d, i))
            if i + 2 <= self.n - 2:
                self.send(d, i + 2)


def sent(buf, send_sem, recv_sem, peer):
    pltpu.make_async_remote_copy(
        src_ref=buf, dst_ref=buf, send_sem=send_sem, recv_sem=recv_sem,
        device_id=peer, device_id_type=pl.DeviceIdType.MESH).wait_send()


def trunk_kernel(nz, ny, nx, n_total, x_hbm, w1_hbm, w2_hbm, ht_ref, lab_ref,
                 a_out, g1_out, g2_out,
                 xd, w1_v, w2_v, ht_v, hb, gg2, gg1, ut_v, sl_v, xt_v, da, ecol,
                 rya, ryb, ryc, ryd, rz1, rz2, ry2, agm, zrow, logit,
                 d1, d2, r1, r2, gram_d, gram_m, m1, m2,
                 sya, vya, syb, vyb, syc, vyc, syd, vyd, sz1, vz1, sz2, vz2, sy2, vy2, sam, vam,
                 w_sem, x_sem, sd, vd, sx, vx, sgd, vgd, sgm, vgm, o_sem):
    me = lax.axis_index('model')
    dat = lax.axis_index('data')
    z, y = lax.div(me, ny), lax.rem(me, ny)
    x, core = lax.div(dat, CORES), lax.rem(dat, CORES)
    n_model, nd = nz * ny, nx * CORES
    rows, n_dim = gg2.shape[2], gg2.shape[3]
    n_tok, n_ffn = sl_v.shape
    n_task = gg2.shape[0] // CORES
    n_class = ht_ref.shape[0]
    half_rows = rows // 2
    c1 = rya.shape[4]
    blk = ny * rows

    def peer_y(t):
        return (z * ny + t, dat)

    def peer_z(t):
        return (t * ny + y, dat)

    def peer_m(t):
        return (t, dat)

    def peer_d(t):
        return (me, t)

    def peer_x(t):
        return (me, t * CORES + core)

    other = (me, x * CORES + 1 - core)

    def offset(i):
        step = lax.div(i + 1, 2)
        return nz // 2 + jnp.where(lax.rem(i, 2) == 1, -step, step)

    def block_rows(i):
        return pl.ds(pl.multiple_of(lax.rem(z + offset(i), nz) * blk, blk), blk)

    def load_x(i):
        at = block_rows(i)
        return pltpu.make_async_copy(x_hbm.at[at, :], xd.at[at, :], x_sem.at[i])

    load_w1 = pltpu.make_async_copy(w1_hbm, w1_v, w_sem.at[0])
    load_w2 = pltpu.make_async_copy(w2_hbm, w2_v, w_sem.at[1])
    load_w1.start()
    load_x(0).start()
    load_w2.start()

    def start_x(i, _):
        load_x(i).start()
        return 0
    lax.fori_loop(1, nz, start_x, 0)

    barrier = pltpu.get_barrier_semaphore()
    greeted = [peer_d(lax.rem(dat + k, nd)) for k in range(1, nd)]
    greeted += [peer_m(lax.rem(me + k, n_model)) for k in range(1, n_model)]
    for peer in greeted:
        pl.semaphore_signal(barrier, inc=1, device_id=peer, device_id_type=pl.DeviceIdType.MESH)

    def hs(half):
        return pl.ds(half * half_rows, half_rows)

    left, right = pl.ds(0, c1), pl.ds(c1, n_dim - c1)

    def slot(off):
        return 2 * (nz // 2 - off) - 1 if off < nz // 2 else 2 * (off - nz // 2)

    own = slot(0)

    def add_y1(first):
        def add(dest, half, off, buf):
            def body(k, _):
                gg2[first + k, dest, hs(half), left] += buf[k]
                return 0
            lax.fori_loop(0, buf.shape[0], body, 0)
        return add

    def add_z1(dest, half, off, buf):
        gg2[slot(off), y, hs(half), left] += buf[...]

    def add_z2(dest, half, off, buf):
        def body(k, _):
            gg2[slot(off), k, hs(half), right] += buf[k]
            return 0
        lax.fori_loop(0, ny, body, 0)

    def add_y2(dest, half, off, buf):
        gg2[own, dest, hs(half), right] += buf[...]

    def landing(buf):
        return lambda d, i: buf.at[d, i]

    rings = {
        'z1': Ring(nz, z, peer_z, lambda t, h, o: gg2.at[slot(o), y, hs(h), left], landing(rz1), sz1.at[0], vz1, add_z1),
        'z2': Ring(nz, z, peer_z, lambda t, h, o: gg2.at[slot(o), :, hs(h), right], landing(rz2), sz2.at[0], vz2, add_z2),
        'y2': Ring(ny, y, peer_y, lambda t, h, o: gg2.at[own, t, hs(h), right], landing(ry2), sy2.at[0], vy2, add_y2),
    }
    first = 0
    for name, recv, send_sem, recv_sem in (('ya', rya, sya, vya), ('yb', ryb, syb, vyb), ('yc', ryc, syc, vyc), ('yd', ryd, syd, vyd)):
        group = pl.ds(first, recv.shape[2])
        rings[name] = Ring(ny, y, peer_y, lambda t, h, o, group=group: gg2.at[group, t, hs(h), left],
                           landing(recv), send_sem.at[0], recv_sem, add_y1(first))
        first += recv.shape[2]

    scale = np.float32(np.sqrt(2.0 / np.pi))

    def block(i, _):
        load_x(i).wait()
        at = block_rows(i)
        pre = jnp.dot(xd[at, :], w1_v[...], preferred_element_type=F32)
        square = pre * pre
        th = jnp.tanh(scale * (pre + np.float32(0.044715) * (square * pre)))
        cdf = 0.5 * (1.0 + th)
        act = (pre * cdf).astype(BF16)
        sl_v[at, :] = cdf + 0.5 * pre * (1.0 - th * th) * (scale * (1.0 + np.float32(3 * 0.044715) * square))
        ut_v[:, at] = act.T
        part = jnp.dot(act, w2_v[...], preferred_element_type=F32)
        gg2[i] = part.reshape(ny, rows, n_dim)
        return 0

    load_w1.wait()
    load_w2.wait()
    block(0, 0)
    pl.semaphore_wait(barrier, len(greeted))
    rings['z2'].begin(0)
    lax.fori_loop(1, 3, block, 0)
    rings['ya'].begin(0)
    rings['z2'].begin(1)
    rings['ya'].begin(1)
    lax.fori_loop(3, nz, block, 0)

    def flip(i, _):
        at = pl.ds(pl.multiple_of(i * blk, blk), blk)
        xt_v[:, at] = xd[at, :].T
        return 0
    lax.fori_loop(0, nz, flip, 0)
    ht_v[...] = jnp.zeros_like(ht_v)
    for c in range(n_class):
        ht_v[4 * c:4 * c + n_task, :] = ht_ref[c].astype(F32)
        for t in range(n_task):
            hb[4 * c + t] = jnp.broadcast_to(ht_ref[c, t:t + 1, :].astype(F32), (8, n_dim))

    order = [
        ('z2', 0), ('ya', 0), ('z2', 1), ('z2', 2), ('ya', 1), ('z2', 3), ('ya', 2), ('z2', 4), ('yb', 0), ('z1', 0),
        ('yb', 1), ('z2', 5), ('yb', 2), ('z1', 1), ('yc', 0), ('yc', 1), ('z1', 2), ('z2', 6), ('yc', 2), ('z1', 3),
        ('z1', 4), ('yd', 0), ('yd', 1), ('yd', 2), ('z1', 5), ('y2', 0), ('y2', 1), ('z1', 6), ('y2', 2)]
    begins = {('ya', 0): 'yb', ('ya', 2): 'z1', ('yb', 0): 'yc', ('yc', 0): 'yd', ('yd', 0): 'y2'}
    for event in order:
        name, i = event
        rings[name].step(i)
        if event in begins:
            rings[begins[event]].begin(0)
            rings[begins[event]].begin(1)

    mine = pl.ds(pl.multiple_of(me * rows, rows), rows)
    zrow[...] = (xd[mine, :].astype(F32) + gg2[own, y]).astype(BF16)
    logit[...] = lax.dot_general(ht_v[...].astype(BF16), zrow[...], (((1,), (1,)), ((), ())), preferred_element_type=F32)
    per = 128 // rows
    wide = lab_ref[:, pl.ds(pl.multiple_of(lax.div(me, per) * 128, 128), 128)]
    lab = wide[:, :rows]
    for k in range(1, per):
        lab = jnp.where(lax.rem(me, per) == k, wide[:, k * rows:(k + 1) * rows], lab)
    agm[me] = jnp.zeros((8, 128), F32)
    for t in range(n_task):
        ls = [logit[4 * c + t:4 * c + t + 1, :] for c in range(n_class)]
        top = functools.reduce(jnp.maximum, ls)
        es = [jnp.exp(v - top) for v in ls]
        total = functools.reduce(jnp.add, es)
        for c in range(n_class):
            row, first = 2 * c + t // 2, t % 2 * rows
            agm[me, row:row + 1, first:first + rows] = (
                es[c] / total - jnp.where(lab[t:t + 1, :] == c, 1.0, 0.0)) / n_total

    def exchange(n, pos, peer, buf, send_sem, recv_sem, use):
        def copy(k, src):
            return pltpu.make_async_remote_copy(
                src_ref=buf.at[pos], dst_ref=buf.at[src], send_sem=send_sem.at[0], recv_sem=recv_sem.at[k],
                device_id=peer(lax.rem(pos + k, n)), device_id_type=pl.DeviceIdType.MESH)
        for k in range(1, n):
            copy(k, pos).start()
        use(pos)
        for k in range(1, n):
            src = lax.rem(pos + n - k, n)
            copy(k, src).wait_recv()
            use(src)

    def turn(k):
        ecol[k] = agm[k].T

    exchange(n_model, me, peer_m, agm, sam, vam, turn)
    for buf, send_sem, recv_sem in ((rya, sya, vya), (ryb, syb, vyb), (ryc, syc, vyc), (ryd, syd, vyd),
                                    (rz1, sz1, vz1), (rz2, sz2, vz2), (ry2, sy2, vy2)):
        sent(buf, send_sem.at[0], recv_sem.at[0, 0], other)

    def make_dz(t, cols):
        def body(i, _):
            at = pl.ds(pl.multiple_of(i * rows, rows), rows)
            first = t % 2 * rows
            es = [jnp.broadcast_to(ecol[i, first:first + rows, 2 * c + t // 2:2 * c + t // 2 + 1], (rows, 128))
                  for c in range(n_class)]
            for j in range(cols[0], cols[1], 128):
                parts = [es[c] * jnp.concatenate([hb[4 * c + t, :, j:j + 128]] * (rows // 8), axis=0)
                         for c in range(n_class)]
                xd[at, j:j + 128] = functools.reduce(jnp.add, parts).astype(BF16)
            return 0
        lax.fori_loop(0, n_model, body, 0, unroll=4)

    tile = 256
    q1 = gg1.shape[2]

    def make_g2(t, cols):
        def body(i, _):
            at = pl.ds(pl.multiple_of(i * tile, tile), tile)
            out = jnp.dot(ut_v[...], xd[:, at], preferred_element_type=F32).reshape(nx, CORES, rows, tile)
            for c in range(CORES):
                gg2[CORES * t + c, :, :, at] = out[:, c]
            return 0
        lax.fori_loop(cols[0] // tile, cols[1] // tile, body, 0)

    def make_da(part):
        def body(i, _):
            at = pl.ds(pl.multiple_of(i * 2 * tile, 2 * tile), 2 * tile)
            out = lax.dot_general(xd[at, :], w2_v[...], (((1,), (1,)), ((), ())), preferred_element_type=F32)
            da[at, :] = (out * sl_v[at, :]).astype(BF16)
            return 0
        n_half = n_tok // (4 * tile)
        lax.fori_loop(part * n_half, (part + 1) * n_half, body, 0)

    def make_g1(t):
        hx = nx // 2

        def body(i, _):
            at = pl.ds(pl.multiple_of(i * tile, tile), tile)
            for k in (0, 1):
                part = pl.ds(k * (n_dim // 2), n_dim // 2)
                out = jnp.dot(xt_v[part, :], da[:, at], preferred_element_type=F32).reshape(hx, CORES, q1, tile)
                for c in range(CORES):
                    gg1[CORES * t + c, k * hx:(k + 1) * hx, :, at] = out[:, c]
            return 0
        lax.fori_loop(0, n_ffn // tile, body, 0)

    all1, all2 = (0, n_ffn), (0, n_dim)
    stages = [(2, 0, (0, n_dim // 2)), (2, 0, (n_dim // 2, n_dim)), (1, 0, all1)]
    for t in range(1, n_task):
        stages += [(2, t, all2), (1, t, all1)]
    n_stage = len(stages)
    sets = {2: (gg2, d2, r2), 1: (gg1, d1, r1)}

    def columns(s):
        first, last = stages[s][2]
        return pl.ds(first, last - first)

    def swap(s):
        g, buf, _ = sets[stages[s][0]]
        t = stages[s][1]
        return pltpu.make_async_remote_copy(
            src_ref=g.at[CORES * t + 1 - core, :, :, columns(s)], dst_ref=buf.at[t, :, :, columns(s)],
            send_sem=sd.at[stages[s][0] - 1], recv_sem=vd.at[s], device_id=other, device_id_type=pl.DeviceIdType.MESH)

    def ring_of(s):
        g, _, r = sets[stages[s][0]]
        t = stages[s][1]
        half = g.shape[2] // 2

        def chunk(dest, h, off):
            return g.at[CORES * t + core, dest, pl.ds(h * half, half), columns(s)]

        def add(dest, h, off, buf):
            g[CORES * t + core, dest, pl.ds(h * half, half), columns(s)] += buf[...]

        def into(d, i):
            return r.at[t, d, i, :, columns(s)]

        return Ring(nx, x, peer_x, chunk, into, sx.at[stages[s][0] - 1], vx.at[s], add)

    def launch(s):
        g, buf, _ = sets[stages[s][0]]
        t = stages[s][1]
        swap(s).wait_recv()

        def body(k, _):
            g[CORES * t + core, k, :, columns(s)] += buf[t, k, :, columns(s)]
            return 0
        lax.fori_loop(0, nx, body, 0)
        if s >= 4:
            ring_of(s - 2).step(0)
        ring_of(s).begin(0)
        ring_of(s).begin(1)

    for s in range(n_stage):
        which, t, cols = stages[s]
        if which == 2:
            make_dz(t, cols)
            if s >= 1:
                launch(s - 1)
            make_g2(t, cols)
        else:
            make_da(0)
            launch(s - 1)
            make_da(1)
            if s == 2:
                ring_of(0).step(0)
            make_g1(t)
            if s == 2:
                ring_of(1).step(0)
        swap(s).start()
    launch(n_stage - 1)
    for s in (n_stage - 2, n_stage - 1):
        ring_of(s).step(0)
    for s in range(n_stage):
        ring_of(s).step(1)
        ring_of(s).step(2)

    pairs = [(i, j) for i in range(n_task) for j in range(i, n_task)]

    def fold(g, accs):
        width = g.shape[3]

        def body(k, accs):
            at = pl.ds(pl.multiple_of(k * 8, 8), 8)
            vals = [g[CORES * t + core, x, at, :] for t in range(n_task)]
            return tuple(acc + sum((vals[i] * vals[j])[:, w:w + 128] for w in range(0, width, 128))
                         for acc, (i, j) in zip(accs, pairs))
        return lax.fori_loop(0, g.shape[2] // 8, body, accs)

    accs = tuple(jnp.zeros((8, 128), F32) for _ in pairs)
    accs = fold(gg2, accs)
    accs = fold(gg1, accs)
    lane = lax.broadcasted_iota(jnp.int32, (1, 128), 1)
    part = jnp.zeros((1, 128), F32)
    for acc, (i, j) in zip(accs, pairs):
        hit = (lane == n_task * i + j) | (lane == n_task * j + i)
        part = jnp.where(hit, jnp.sum(jnp.sum(acc, axis=0, keepdims=True), axis=1, keepdims=True), part)

    def all_sum(n, pos, peer, buf, send_sem, recv_sem, val):
        buf[pos, 0:1, :] = val
        for k in range(1, n):
            pltpu.make_async_remote_copy(
                src_ref=buf.at[pos, pl.ds(0, 1), :], dst_ref=buf.at[pos, pl.ds(0, 1), :],
                send_sem=send_sem.at[0], recv_sem=recv_sem.at[0],
                device_id=peer(lax.rem(pos + k, n)), device_id_type=pl.DeviceIdType.MESH).start()
        rest = buf.at[pl.ds(0, n - 1), pl.ds(0, 1), :]
        pltpu.make_async_remote_copy(
            src_ref=rest, dst_ref=rest, send_sem=send_sem.at[0], recv_sem=recv_sem.at[0],
            device_id=other, device_id_type=pl.DeviceIdType.MESH).wait_recv()
        out = buf[0, 0:1, :]
        for k in range(1, n):
            out = out + buf[k, 0:1, :]
        return out

    part = all_sum(nd, dat, peer_d, gram_d, sgd, vgd, part)
    part = all_sum(n_model, me, peer_m, gram_m, sgm, vgm, part)

    gram = [[jnp.broadcast_to(part[:, n_task * i + j:n_task * i + j + 1], (1, 128)) for j in range(n_task)]
            for i in range(n_task)]
    trace_scale = functools.reduce(jnp.add, [gram[i][i] for i in range(n_task)]) / n_task

    def eg(i, ws):
        ups = []
        for t in range(n_task):
            prod = functools.reduce(jnp.add, [gram[t][j] * ws[j] for j in range(n_task)])
            ups.append(ws[t] * jnp.exp(-prod / trace_scale))
        total = functools.reduce(jnp.add, ups)
        return tuple(up / total for up in ups)

    ws = tuple(jnp.full((1, 128), 1.0 / n_task, F32) for _ in range(n_task))
    ws = lax.fori_loop(0, STEPS, eg, ws)
    weights = jnp.zeros((1, 128), F32)
    for t in range(n_task):
        weights = jnp.where(lane == t, ws[t], weights)
    a_out[0:1, :] = weights
    writes = []

    def mix(g, out):
        width = g.shape[3]

        def body(k, _):
            at = pl.ds(pl.multiple_of(k * 8, 8), 8)
            for w in range(0, width, 128):
                acc = ws[0] * g[core, x, at, w:w + 128]
                for t in range(1, n_task):
                    acc = acc + ws[t] * g[CORES * t + core, x, at, w:w + 128]
                out[at, w:w + 128] = acc
            return 0
        lax.fori_loop(0, g.shape[2] // 8, body, 0)
    for k, (g, stage_out, out) in enumerate(((gg1, m1, g1_out), (gg2, m2, g2_out))):
        mix(g, stage_out)
        writes.append(pltpu.make_async_copy(stage_out, out, o_sem.at[k]))
        writes[-1].start()

    for c in writes:
        c.wait()
    sent(agm.at[pl.ds(0, n_model - 1)], sam.at[0], vam.at[0], other)
    sent(gram_d.at[pl.ds(0, nd - 1), pl.ds(0, 1), :], sgd.at[0], vgd.at[0], other)
    sent(gram_m.at[pl.ds(0, n_model - 1), pl.ds(0, 1), :], sgm.at[0], vgm.at[0], other)
    for k, (d, r) in enumerate(((d1, r1), (d2, r2))):
        sent(d, sd.at[k], vd.at[0], other)
        sent(r, sx.at[k], vx.at[0, 0, 0], other)


def write_kernel(a_ref, g1_ref, g2_ref, a_out, g1_out, g2_out):
    a_out[...] = a_ref[0:1, 0:a_out.shape[1]]
    g1_out[...] = g1_ref[...]
    g2_out[...] = g2_ref[...]


def solution(mesh, ny=NY):
    n_data = mesh.shape['data']
    n_model = mesh.shape['model']
    nz = n_model // ny
    nx = n_data // CORES

    def local_step(tokens, w_up, w_down, task_heads, labels):
        n_tok, n_dim = tokens.shape
        n_ffn = w_up.shape[1]
        n_task, _, n_class = task_heads.shape
        rows = n_tok // n_model
        hr = rows // 2
        c1 = 5 * n_dim // 8
        c2 = n_dim - c1
        f1 = n_dim // n_data
        f2 = n_ffn // n_data
        heads = jnp.transpose(task_heads, (2, 0, 1))
        vm = pl.BlockSpec(memory_space=pltpu.VMEM)
        hbm = pl.BlockSpec(memory_space=pl.ANY)
        dma = pltpu.SemaphoreType.DMA
        outs = [jax.ShapeDtypeStruct((f1, n_ffn), F32), jax.ShapeDtypeStruct((f2, n_dim), F32)]
        stages = 2 * n_task + 1

        results = pl.pallas_call(
            functools.partial(trunk_kernel, nz, ny, nx, n_tok * n_data),
            out_shape=[jax.ShapeDtypeStruct((8, 128), F32)] + outs,
            in_specs=[hbm] * 3 + [vm] * 2, out_specs=[vm, hbm, hbm],
            scratch_shapes=[
                pltpu.VMEM((n_tok, n_dim), BF16), pltpu.VMEM((n_dim, n_ffn), BF16), pltpu.VMEM((n_ffn, n_dim), BF16),
                pltpu.VMEM((16, n_dim), F32), pltpu.VMEM((n_class * n_task, 8, n_dim), F32),
                pltpu.VMEM((CORES * n_task, nx, f2, n_dim), F32), pltpu.VMEM((CORES * n_task, nx, f1, n_ffn), F32),
                pltpu.VMEM((n_ffn, n_tok), BF16), pltpu.VMEM((n_tok, n_ffn), F32), pltpu.VMEM((n_dim, n_tok), BF16),
                pltpu.VMEM((n_tok, n_ffn), BF16), pltpu.VMEM((n_model, 128, 8), F32),
                pltpu.VMEM((2, ny - 1, 3, hr, c1), F32), pltpu.VMEM((2, ny - 1, nz - 6, hr, c1), F32),
                pltpu.VMEM((2, ny - 1, 2, hr, c1), F32), pltpu.VMEM((2, ny - 1, 1, hr, c1), F32),
                pltpu.VMEM((2, nz - 1, hr, c1), F32),
                pltpu.VMEM((2, nz - 1, ny, hr, c2), F32), pltpu.VMEM((2, ny - 1, hr, c2), F32),
                pltpu.VMEM((n_model, 8, 128), F32),
                pltpu.VMEM((rows, n_dim), BF16), pltpu.VMEM((16, rows), F32),
                pltpu.VMEM((n_task, nx, f1, n_ffn), F32), pltpu.VMEM((n_task, nx, f2, n_dim), F32),
                pltpu.VMEM((n_task, 2, nx - 1, f1 // 2, n_ffn), F32), pltpu.VMEM((n_task, 2, nx - 1, f2 // 2, n_dim), F32),
                pltpu.VMEM((n_data, 8, 128), F32), pltpu.VMEM((n_model, 8, 128), F32),
                pltpu.VMEM((f1, n_ffn), F32), pltpu.VMEM((f2, n_dim), F32),
                *[dma((1,)), dma((2, ny - 1))] * 4, dma((1,)), dma((2, nz - 1)),
                dma((1,)), dma((2, nz - 1)), dma((1,)), dma((2, ny - 1)),
                dma((1,)), dma((n_model,)),
                dma((2,)), dma((nz,)), dma((2,)), dma((stages,)), dma((2,)), dma((stages, 2, nx - 1)),
                dma((1,)), dma((1,)), dma((1,)), dma((1,)), dma((2,))],
            compiler_params=pltpu.CompilerParams(collective_id=0, has_side_effects=True, vmem_limit_bytes=VMEM_LIMIT),
            name='trunk',
        )(tokens, w_up, w_down, heads, labels)
        weights, g1, g2 = pl.pallas_call(
            write_kernel, out_shape=[jax.ShapeDtypeStruct((1, n_task), F32)] + outs,
            in_specs=[vm] * 3, out_specs=[vm] * 3, name='write',
        )(*results)
        return weights.reshape(n_task), g1, g2

    return jax.shard_map(
        local_step, mesh=mesh,
        in_specs=(P('data', None), P(None, 'model'), P('model', None), P(None, None, None), P(None, 'data')),
        out_specs=(P(None), P('data', 'model'), P(('model', 'data'), None)),
        check_vma=False)
```

```python
import functools

import jax
import jax.numpy as jnp
import numpy as np
from jax import lax
from jax.experimental import pallas as pl
from jax.experimental.pallas import tpu as pltpu
from jax.sharding import PartitionSpec as P

STEPS = 20
NY = 4
CORES = 2
F32 = jnp.float32
BF16 = jnp.bfloat16
VMEM_LIMIT = 67043328


def chain(n):
    return [(i % 2 == 0, n // 2 - (i + 1) // 2) for i in range(n - 1)]


class Ring:
    def __init__(self, n, me, peer, chunk, recv, send_sem, recv_sem, add):
        self.n, self.me, self.peer, self.chunk = n, me, peer, chunk
        self.recv, self.send_sem, self.recv_sem, self.add = recv, send_sem, recv_sem, add
        self.order = chain(n)

    def copy(self, d, i):
        far, dist = self.order[i]
        sign = 1 if d == 0 else -1
        half = d if far else 1 - d
        dest = lax.rem(self.me + self.n + sign * dist, self.n)
        target = lax.rem(self.me + self.n + sign, self.n)
        return pltpu.make_async_remote_copy(
            src_ref=self.chunk(dest, half, sign * dist % self.n), dst_ref=self.recv(d, i),
            send_sem=self.send_sem, recv_sem=self.recv_sem.at[d, i],
            device_id=self.peer(target), device_id_type=pl.DeviceIdType.MESH)

    def send(self, d, i):
        self.copy(d, i).start()

    def begin(self, i):
        for d in (0, 1):
            self.send(d, i)

    def step(self, i):
        for d in (0, 1):
            far, dist = self.order[i]
            sign = 1 if d == 0 else -1
            half = d if far else 1 - d
            self.copy(d, i).wait_recv()
            dest = lax.rem(self.me + self.n + sign * (dist - 1), self.n)
            self.add(dest, half, sign * (dist - 1) % self.n, self.recv(d, i))
            if i + 2 <= self.n - 2:
                self.send(d, i + 2)


def sent(buf, send_sem, recv_sem, peer):
    pltpu.make_async_remote_copy(
        src_ref=buf, dst_ref=buf, send_sem=send_sem, recv_sem=recv_sem,
        device_id=peer, device_id_type=pl.DeviceIdType.MESH).wait_send()


def trunk_kernel(nz, ny, nx, n_total, x_hbm, w1_hbm, w2_hbm, ht_ref, lab_ref,
                 a_out, g1_out, g2_out,
                 xd, w1_v, w2_v, ht_v, hb, gg2, gg1, ut_v, sl_v, xt_v, da, ecol,
                 rya, ryb, ryc, ryd, rz1, rz2, ry2, agm, zrow, logit,
                 d1, d2, r1, r2, gram_d, gram_m, m1, m2,
                 sya, vya, syb, vyb, syc, vyc, syd, vyd, sz1, vz1, sz2, vz2, sy2, vy2, sam, vam,
                 w_sem, x_sem, sd, vd, sx, vx, sgd, vgd, sgm, vgm, o_sem):
    me = lax.axis_index('model')
    dat = lax.axis_index('data')
    z, y = lax.div(me, ny), lax.rem(me, ny)
    x, core = lax.div(dat, CORES), lax.rem(dat, CORES)
    n_model, nd = nz * ny, nx * CORES
    rows, n_dim = gg2.shape[2], gg2.shape[3]
    n_tok, n_ffn = sl_v.shape
    n_task = gg2.shape[0] // CORES
    n_class = ht_ref.shape[0]
    half_rows = rows // 2
    c1 = rya.shape[4]
    blk = ny * rows

    def peer_y(t):
        return (z * ny + t, dat)

    def peer_z(t):
        return (t * ny + y, dat)

    def peer_m(t):
        return (t, dat)

    def peer_d(t):
        return (me, t)

    def peer_x(t):
        return (me, t * CORES + core)

    other = (me, x * CORES + 1 - core)

    def offset(i):
        step = lax.div(i + 1, 2)
        return nz // 2 + jnp.where(lax.rem(i, 2) == 1, -step, step)

    def block_rows(i):
        return pl.ds(pl.multiple_of(lax.rem(z + offset(i), nz) * blk, blk), blk)

    def load_x(i):
        at = block_rows(i)
        return pltpu.make_async_copy(x_hbm.at[at, :], xd.at[at, :], x_sem.at[i])

    load_w1 = pltpu.make_async_copy(w1_hbm, w1_v, w_sem.at[0])
    load_w2 = pltpu.make_async_copy(w2_hbm, w2_v, w_sem.at[1])
    load_w1.start()
    load_x(0).start()
    load_w2.start()

    def start_x(i, _):
        load_x(i).start()
        return 0
    lax.fori_loop(1, nz, start_x, 0)

    barrier = pltpu.get_barrier_semaphore()
    greeted = [peer_d(lax.rem(dat + k, nd)) for k in range(1, nd)]
    greeted += [peer_m(lax.rem(me + k, n_model)) for k in range(1, n_model)]
    for peer in greeted:
        pl.semaphore_signal(barrier, inc=1, device_id=peer, device_id_type=pl.DeviceIdType.MESH)

    def hs(half):
        return pl.ds(half * half_rows, half_rows)

    left, right = pl.ds(0, c1), pl.ds(c1, n_dim - c1)

    def slot(off):
        return 2 * (nz // 2 - off) - 1 if off < nz // 2 else 2 * (off - nz // 2)

    own = slot(0)

    def add_y1(first):
        def add(dest, half, off, buf):
            def body(k, _):
                gg2[first + k, dest, hs(half), left] += buf[k]
                return 0
            lax.fori_loop(0, buf.shape[0], body, 0)
        return add

    def add_z1(dest, half, off, buf):
        gg2[slot(off), y, hs(half), left] += buf[...]

    def add_z2(dest, half, off, buf):
        def body(k, _):
            gg2[slot(off), k, hs(half), right] += buf[k]
            return 0
        lax.fori_loop(0, ny, body, 0)

    def add_y2(dest, half, off, buf):
        gg2[own, dest, hs(half), right] += buf[...]

    def landing(buf):
        return lambda d, i: buf.at[d, i]

    rings = {
        'z1': Ring(nz, z, peer_z, lambda t, h, o: gg2.at[slot(o), y, hs(h), left], landing(rz1), sz1.at[0], vz1, add_z1),
        'z2': Ring(nz, z, peer_z, lambda t, h, o: gg2.at[slot(o), :, hs(h), right], landing(rz2), sz2.at[0], vz2, add_z2),
        'y2': Ring(ny, y, peer_y, lambda t, h, o: gg2.at[own, t, hs(h), right], landing(ry2), sy2.at[0], vy2, add_y2),
    }
    first = 0
    for name, recv, send_sem, recv_sem in (('ya', rya, sya, vya), ('yb', ryb, syb, vyb), ('yc', ryc, syc, vyc), ('yd', ryd, syd, vyd)):
        group = pl.ds(first, recv.shape[2])
        rings[name] = Ring(ny, y, peer_y, lambda t, h, o, group=group: gg2.at[group, t, hs(h), left],
                           landing(recv), send_sem.at[0], recv_sem, add_y1(first))
        first += recv.shape[2]

    scale = np.float32(np.sqrt(2.0 / np.pi))

    def block(i, _):
        load_x(i).wait()
        at = block_rows(i)
        pre = jnp.dot(xd[at, :], w1_v[...], preferred_element_type=F32)
        square = pre * pre
        th = jnp.tanh(scale * (pre + np.float32(0.044715) * (square * pre)))
        cdf = 0.5 * (1.0 + th)
        act = (pre * cdf).astype(BF16)
        sl_v[at, :] = cdf + 0.5 * pre * (1.0 - th * th) * (scale * (1.0 + np.float32(3 * 0.044715) * square))
        ut_v[:, at] = act.T
        part = jnp.dot(act, w2_v[...], preferred_element_type=F32)
        gg2[i] = part.reshape(ny, rows, n_dim)
        return 0

    load_w1.wait()
    load_w2.wait()
    block(0, 0)
    pl.semaphore_wait(barrier, len(greeted))
    rings['z2'].begin(0)
    lax.fori_loop(1, 3, block, 0)
    rings['ya'].begin(0)
    rings['z2'].begin(1)
    rings['ya'].begin(1)
    lax.fori_loop(3, nz, block, 0)

    def flip(i, _):
        at = pl.ds(pl.multiple_of(i * blk, blk), blk)
        xt_v[:, at] = xd[at, :].T
        return 0
    lax.fori_loop(0, nz, flip, 0)
    ht_v[...] = jnp.zeros_like(ht_v)
    for c in range(n_class):
        ht_v[4 * c:4 * c + n_task, :] = ht_ref[c].astype(F32)
        for t in range(n_task):
            hb[4 * c + t] = jnp.broadcast_to(ht_ref[c, t:t + 1, :].astype(F32), (8, n_dim))

    order = [
        ('z2', 0), ('ya', 0), ('z2', 1), ('z2', 2), ('ya', 1), ('z2', 3), ('ya', 2), ('yb', 0), ('z2', 4), ('z1', 0),
        ('yb', 1), ('z2', 5), ('yb', 2), ('z1', 1), ('yc', 0), ('z2', 6), ('yc', 1), ('z1', 2), ('yc', 2), ('z1', 3),
        ('z1', 4), ('yd', 0), ('yd', 1), ('y2', 0), ('y2', 1), ('yd', 2), ('z1', 5), ('z1', 6), ('y2', 2)]
    begins = {('ya', 0): 'yb', ('ya', 2): 'z1', ('yb', 0): 'yc', ('yc', 0): 'yd', ('z2', 6): 'y2'}
    for event in order:
        name, i = event
        rings[name].step(i)
        if event in begins:
            rings[begins[event]].begin(0)
            rings[begins[event]].begin(1)

    mine = pl.ds(pl.multiple_of(me * rows, rows), rows)
    zrow[...] = (xd[mine, :].astype(F32) + gg2[own, y]).astype(BF16)
    logit[...] = lax.dot_general(ht_v[...].astype(BF16), zrow[...], (((1,), (1,)), ((), ())), preferred_element_type=F32)
    per = 128 // rows
    wide = lab_ref[:, pl.ds(pl.multiple_of(lax.div(me, per) * 128, 128), 128)]
    lab = wide[:, :rows]
    for k in range(1, per):
        lab = jnp.where(lax.rem(me, per) == k, wide[:, k * rows:(k + 1) * rows], lab)
    agm[me] = jnp.zeros((8, 128), F32)
    for t in range(n_task):
        ls = [logit[4 * c + t:4 * c + t + 1, :] for c in range(n_class)]
        top = functools.reduce(jnp.maximum, ls)
        es = [jnp.exp(v - top) for v in ls]
        total = functools.reduce(jnp.add, es)
        for c in range(n_class):
            row, first = 2 * c + t // 2, t % 2 * rows
            agm[me, row:row + 1, first:first + rows] = (
                es[c] / total - jnp.where(lab[t:t + 1, :] == c, 1.0, 0.0)) / n_total

    def exchange(n, pos, peer, buf, send_sem, recv_sem, use):
        def copy(k, src):
            return pltpu.make_async_remote_copy(
                src_ref=buf.at[pos], dst_ref=buf.at[src], send_sem=send_sem.at[0], recv_sem=recv_sem.at[k],
                device_id=peer(lax.rem(pos + k, n)), device_id_type=pl.DeviceIdType.MESH)
        for k in range(1, n):
            copy(k, pos).start()
        use(pos)
        for k in range(1, n):
            src = lax.rem(pos + n - k, n)
            copy(k, src).wait_recv()
            use(src)

    def turn(k):
        ecol[k] = agm[k].T

    exchange(n_model, me, peer_m, agm, sam, vam, turn)
    for buf, send_sem, recv_sem in ((rya, sya, vya), (ryb, syb, vyb), (ryc, syc, vyc), (ryd, syd, vyd),
                                    (rz1, sz1, vz1), (rz2, sz2, vz2), (ry2, sy2, vy2)):
        sent(buf, send_sem.at[0], recv_sem.at[0, 0], other)

    def make_dz(t, cols):
        def body(i, _):
            at = pl.ds(pl.multiple_of(i * rows, rows), rows)
            first = t % 2 * rows
            es = [jnp.broadcast_to(ecol[i, first:first + rows, 2 * c + t // 2:2 * c + t // 2 + 1], (rows, 128))
                  for c in range(n_class)]
            for j in range(cols[0], cols[1], 128):
                parts = [es[c] * jnp.concatenate([hb[4 * c + t, :, j:j + 128]] * (rows // 8), axis=0)
                         for c in range(n_class)]
                xd[at, j:j + 128] = functools.reduce(jnp.add, parts).astype(BF16)
            return 0
        lax.fori_loop(0, n_model, body, 0, unroll=4)

    tile = 256
    q1 = gg1.shape[2]

    def make_g2(t, cols):
        def body(i, _):
            at = pl.ds(pl.multiple_of(i * tile, tile), tile)
            out = jnp.dot(ut_v[...], xd[:, at], preferred_element_type=F32).reshape(nx, CORES, rows, tile)
            for c in range(CORES):
                gg2[CORES * t + c, :, :, at] = out[:, c]
            return 0
        lax.fori_loop(cols[0] // tile, cols[1] // tile, body, 0)

    def make_da(part):
        def body(i, _):
            at = pl.ds(pl.multiple_of(i * 2 * tile, 2 * tile), 2 * tile)
            out = lax.dot_general(xd[at, :], w2_v[...], (((1,), (1,)), ((), ())), preferred_element_type=F32)
            da[at, :] = (out * sl_v[at, :]).astype(BF16)
            return 0
        n_half = n_tok // (4 * tile)
        lax.fori_loop(part * n_half, (part + 1) * n_half, body, 0)

    def make_g1(t):
        hx = nx // 2

        def body(i, _):
            at = pl.ds(pl.multiple_of(i * tile, tile), tile)
            for k in (0, 1):
                part = pl.ds(k * (n_dim // 2), n_dim // 2)
                out = jnp.dot(xt_v[part, :], da[:, at], preferred_element_type=F32).reshape(hx, CORES, q1, tile)
                for c in range(CORES):
                    gg1[CORES * t + c, k * hx:(k + 1) * hx, :, at] = out[:, c]
            return 0
        lax.fori_loop(0, n_ffn // tile, body, 0)

    all1, all2 = (0, n_ffn), (0, n_dim)
    stages = [(2, 0, (0, n_dim // 2)), (2, 0, (n_dim // 2, n_dim)), (1, 0, all1)]
    for t in range(1, n_task):
        stages += [(2, t, all2), (1, t, all1)]
    n_stage = len(stages)
    sets = {2: (gg2, d2, r2), 1: (gg1, d1, r1)}

    def columns(s):
        first, last = stages[s][2]
        return pl.ds(first, last - first)

    def swap(s):
        g, buf, _ = sets[stages[s][0]]
        t = stages[s][1]
        return pltpu.make_async_remote_copy(
            src_ref=g.at[CORES * t + 1 - core, :, :, columns(s)], dst_ref=buf.at[t, :, :, columns(s)],
            send_sem=sd.at[stages[s][0] - 1], recv_sem=vd.at[s], device_id=other, device_id_type=pl.DeviceIdType.MESH)

    def ring_of(s):
        g, _, r = sets[stages[s][0]]
        t = stages[s][1]
        half = g.shape[2] // 2

        def chunk(dest, h, off):
            return g.at[CORES * t + core, dest, pl.ds(h * half, half), columns(s)]

        def add(dest, h, off, buf):
            g[CORES * t + core, dest, pl.ds(h * half, half), columns(s)] += buf[...]

        def into(d, i):
            return r.at[t, d, i, :, columns(s)]

        return Ring(nx, x, peer_x, chunk, into, sx.at[stages[s][0] - 1], vx.at[s], add)

    def launch(s):
        g, buf, _ = sets[stages[s][0]]
        t = stages[s][1]
        swap(s).wait_recv()

        def body(k, _):
            g[CORES * t + core, k, :, columns(s)] += buf[t, k, :, columns(s)]
            return 0
        lax.fori_loop(0, nx, body, 0)
        if s >= 5:
            ring_of(s - 2).step(0)
        ring_of(s).begin(0)
        ring_of(s).begin(1)

    for s in range(n_stage):
        which, t, cols = stages[s]
        if which == 2:
            make_dz(t, cols)
            if s >= 1:
                launch(s - 1)
            make_g2(t, cols)
        else:
            make_da(0)
            launch(s - 1)
            make_da(1)
            if s == 2:
                ring_of(0).step(0)
            make_g1(t)
            if s == 2:
                ring_of(1).step(0)
            if s == 4:
                ring_of(2).step(0)
        swap(s).start()
    launch(n_stage - 1)
    for s in (n_stage - 2, n_stage - 1):
        ring_of(s).step(0)
    for s in range(n_stage):
        ring_of(s).step(1)
        ring_of(s).step(2)

    pairs = [(i, j) for i in range(n_task) for j in range(i, n_task)]

    def fold(g, accs):
        width = g.shape[3]

        def body(k, accs):
            at = pl.ds(pl.multiple_of(k * 8, 8), 8)
            vals = [g[CORES * t + core, x, at, :] for t in range(n_task)]
            return tuple(acc + sum((vals[i] * vals[j])[:, w:w + 128] for w in range(0, width, 128))
                         for acc, (i, j) in zip(accs, pairs))
        return lax.fori_loop(0, g.shape[2] // 8, body, accs)

    accs = tuple(jnp.zeros((8, 128), F32) for _ in pairs)
    accs = fold(gg2, accs)
    accs = fold(gg1, accs)
    lane = lax.broadcasted_iota(jnp.int32, (1, 128), 1)
    part = jnp.zeros((1, 128), F32)
    for acc, (i, j) in zip(accs, pairs):
        hit = (lane == n_task * i + j) | (lane == n_task * j + i)
        part = jnp.where(hit, jnp.sum(jnp.sum(acc, axis=0, keepdims=True), axis=1, keepdims=True), part)

    def all_sum(n, pos, peer, buf, send_sem, recv_sem, val):
        buf[pos, 0:1, :] = val
        for k in range(1, n):
            pltpu.make_async_remote_copy(
                src_ref=buf.at[pos, pl.ds(0, 1), :], dst_ref=buf.at[pos, pl.ds(0, 1), :],
                send_sem=send_sem.at[0], recv_sem=recv_sem.at[0],
                device_id=peer(lax.rem(pos + k, n)), device_id_type=pl.DeviceIdType.MESH).start()
        rest = buf.at[pl.ds(0, n - 1), pl.ds(0, 1), :]
        pltpu.make_async_remote_copy(
            src_ref=rest, dst_ref=rest, send_sem=send_sem.at[0], recv_sem=recv_sem.at[0],
            device_id=other, device_id_type=pl.DeviceIdType.MESH).wait_recv()
        out = buf[0, 0:1, :]
        for k in range(1, n):
            out = out + buf[k, 0:1, :]
        return out

    part = all_sum(nd, dat, peer_d, gram_d, sgd, vgd, part)
    part = all_sum(n_model, me, peer_m, gram_m, sgm, vgm, part)

    gram = [[jnp.broadcast_to(part[:, n_task * i + j:n_task * i + j + 1], (1, 128)) for j in range(n_task)]
            for i in range(n_task)]
    trace_scale = functools.reduce(jnp.add, [gram[i][i] for i in range(n_task)]) / n_task

    def eg(i, ws):
        ups = []
        for t in range(n_task):
            prod = functools.reduce(jnp.add, [gram[t][j] * ws[j] for j in range(n_task)])
            ups.append(ws[t] * jnp.exp(-prod / trace_scale))
        total = functools.reduce(jnp.add, ups)
        return tuple(up / total for up in ups)

    ws = tuple(jnp.full((1, 128), 1.0 / n_task, F32) for _ in range(n_task))
    ws = lax.fori_loop(0, STEPS, eg, ws)
    weights = jnp.zeros((1, 128), F32)
    for t in range(n_task):
        weights = jnp.where(lane == t, ws[t], weights)
    a_out[0:1, :] = weights
    writes = []

    def mix(g, out):
        width = g.shape[3]

        def body(k, _):
            at = pl.ds(pl.multiple_of(k * 8, 8), 8)
            for w in range(0, width, 128):
                acc = ws[0] * g[core, x, at, w:w + 128]
                for t in range(1, n_task):
                    acc = acc + ws[t] * g[CORES * t + core, x, at, w:w + 128]
                out[at, w:w + 128] = acc
            return 0
        lax.fori_loop(0, g.shape[2] // 8, body, 0)
    for k, (g, stage_out, out) in enumerate(((gg1, m1, g1_out), (gg2, m2, g2_out))):
        mix(g, stage_out)
        writes.append(pltpu.make_async_copy(stage_out, out, o_sem.at[k]))
        writes[-1].start()

    for c in writes:
        c.wait()
    sent(agm.at[pl.ds(0, n_model - 1)], sam.at[0], vam.at[0], other)
    sent(gram_d.at[pl.ds(0, nd - 1), pl.ds(0, 1), :], sgd.at[0], vgd.at[0], other)
    sent(gram_m.at[pl.ds(0, n_model - 1), pl.ds(0, 1), :], sgm.at[0], vgm.at[0], other)
    for k, (d, r) in enumerate(((d1, r1), (d2, r2))):
        sent(d, sd.at[k], vd.at[0], other)
        sent(r, sx.at[k], vx.at[0, 0, 0], other)


def write_kernel(a_ref, g1_ref, g2_ref, a_out, g1_out, g2_out):
    a_out[...] = a_ref[0:1, 0:a_out.shape[1]]
    g1_out[...] = g1_ref[...]
    g2_out[...] = g2_ref[...]


def solution(mesh, ny=NY):
    n_data = mesh.shape['data']
    n_model = mesh.shape['model']
    nz = n_model // ny
    nx = n_data // CORES

    def local_step(tokens, w_up, w_down, task_heads, labels):
        n_tok, n_dim = tokens.shape
        n_ffn = w_up.shape[1]
        n_task, _, n_class = task_heads.shape
        rows = n_tok // n_model
        hr = rows // 2
        c1 = 5 * n_dim // 8
        c2 = n_dim - c1
        f1 = n_dim // n_data
        f2 = n_ffn // n_data
        heads = jnp.transpose(task_heads, (2, 0, 1))
        vm = pl.BlockSpec(memory_space=pltpu.VMEM)
        hbm = pl.BlockSpec(memory_space=pl.ANY)
        dma = pltpu.SemaphoreType.DMA
        outs = [jax.ShapeDtypeStruct((f1, n_ffn), F32), jax.ShapeDtypeStruct((f2, n_dim), F32)]
        stages = 2 * n_task + 1

        results = pl.pallas_call(
            functools.partial(trunk_kernel, nz, ny, nx, n_tok * n_data),
            out_shape=[jax.ShapeDtypeStruct((8, 128), F32)] + outs,
            in_specs=[hbm] * 3 + [vm] * 2, out_specs=[vm, hbm, hbm],
            scratch_shapes=[
                pltpu.VMEM((n_tok, n_dim), BF16), pltpu.VMEM((n_dim, n_ffn), BF16), pltpu.VMEM((n_ffn, n_dim), BF16),
                pltpu.VMEM((16, n_dim), F32), pltpu.VMEM((n_class * n_task, 8, n_dim), F32),
                pltpu.VMEM((CORES * n_task, nx, f2, n_dim), F32), pltpu.VMEM((CORES * n_task, nx, f1, n_ffn), F32),
                pltpu.VMEM((n_ffn, n_tok), BF16), pltpu.VMEM((n_tok, n_ffn), F32), pltpu.VMEM((n_dim, n_tok), BF16),
                pltpu.VMEM((n_tok, n_ffn), BF16), pltpu.VMEM((n_model, 128, 8), F32),
                pltpu.VMEM((2, ny - 1, 3, hr, c1), F32), pltpu.VMEM((2, ny - 1, nz - 6, hr, c1), F32),
                pltpu.VMEM((2, ny - 1, 2, hr, c1), F32), pltpu.VMEM((2, ny - 1, 1, hr, c1), F32),
                pltpu.VMEM((2, nz - 1, hr, c1), F32),
                pltpu.VMEM((2, nz - 1, ny, hr, c2), F32), pltpu.VMEM((2, ny - 1, hr, c2), F32),
                pltpu.VMEM((n_model, 8, 128), F32),
                pltpu.VMEM((rows, n_dim), BF16), pltpu.VMEM((16, rows), F32),
                pltpu.VMEM((n_task, nx, f1, n_ffn), F32), pltpu.VMEM((n_task, nx, f2, n_dim), F32),
                pltpu.VMEM((n_task, 2, nx - 1, f1 // 2, n_ffn), F32), pltpu.VMEM((n_task, 2, nx - 1, f2 // 2, n_dim), F32),
                pltpu.VMEM((n_data, 8, 128), F32), pltpu.VMEM((n_model, 8, 128), F32),
                pltpu.VMEM((f1, n_ffn), F32), pltpu.VMEM((f2, n_dim), F32),
                *[dma((1,)), dma((2, ny - 1))] * 4, dma((1,)), dma((2, nz - 1)),
                dma((1,)), dma((2, nz - 1)), dma((1,)), dma((2, ny - 1)),
                dma((1,)), dma((n_model,)),
                dma((2,)), dma((nz,)), dma((2,)), dma((stages,)), dma((2,)), dma((stages, 2, nx - 1)),
                dma((1,)), dma((1,)), dma((1,)), dma((1,)), dma((2,))],
            compiler_params=pltpu.CompilerParams(collective_id=0, has_side_effects=True, vmem_limit_bytes=VMEM_LIMIT),
            name='trunk',
        )(tokens, w_up, w_down, heads, labels)
        weights, g1, g2 = pl.pallas_call(
            write_kernel, out_shape=[jax.ShapeDtypeStruct((1, n_task), F32)] + outs,
            in_specs=[vm] * 3, out_specs=[vm] * 3, name='write',
        )(*results)
        return weights.reshape(n_task), g1, g2

    return jax.shard_map(
        local_step, mesh=mesh,
        in_specs=(P('data', None), P(None, 'model'), P('model', None), P(None, None, None), P(None, 'data')),
        out_specs=(P(None), P('data', 'model'), P(('model', 'data'), None)),
        check_vma=False)
```

```python
import functools

import jax
import jax.numpy as jnp
import numpy as np
from jax import lax
from jax.experimental import pallas as pl
from jax.experimental.pallas import tpu as pltpu
from jax.sharding import PartitionSpec as P

STEPS = 20
NY = 4
CORES = 2
F32 = jnp.float32
BF16 = jnp.bfloat16
VMEM_LIMIT = 67043328


def chain(n):
    return [(i % 2 == 0, n // 2 - (i + 1) // 2) for i in range(n - 1)]


class Ring:
    def __init__(self, n, me, peer, chunk, recv, send_sem, recv_sem, add):
        self.n, self.me, self.peer, self.chunk = n, me, peer, chunk
        self.recv, self.send_sem, self.recv_sem, self.add = recv, send_sem, recv_sem, add
        self.order = chain(n)

    def copy(self, d, i):
        far, dist = self.order[i]
        sign = 1 if d == 0 else -1
        half = d if far else 1 - d
        dest = lax.rem(self.me + self.n + sign * dist, self.n)
        target = lax.rem(self.me + self.n + sign, self.n)
        return pltpu.make_async_remote_copy(
            src_ref=self.chunk(dest, half, sign * dist % self.n), dst_ref=self.recv(d, i),
            send_sem=self.send_sem, recv_sem=self.recv_sem.at[d, i],
            device_id=self.peer(target), device_id_type=pl.DeviceIdType.MESH)

    def send(self, d, i):
        self.copy(d, i).start()

    def begin(self, i):
        for d in (0, 1):
            self.send(d, i)

    def step(self, i):
        for d in (0, 1):
            far, dist = self.order[i]
            sign = 1 if d == 0 else -1
            half = d if far else 1 - d
            self.copy(d, i).wait_recv()
            dest = lax.rem(self.me + self.n + sign * (dist - 1), self.n)
            self.add(dest, half, sign * (dist - 1) % self.n, self.recv(d, i))
            if i + 2 <= self.n - 2:
                self.send(d, i + 2)


def sent(buf, send_sem, recv_sem, peer):
    pltpu.make_async_remote_copy(
        src_ref=buf, dst_ref=buf, send_sem=send_sem, recv_sem=recv_sem,
        device_id=peer, device_id_type=pl.DeviceIdType.MESH).wait_send()


def trunk_kernel(nz, ny, nx, n_total, x_hbm, w1_hbm, w2_hbm, ht_ref, lab_ref,
                 a_out, g1_out, g2_out,
                 xd, w1_v, w2_v, ht_v, hb, gg2, gg1, ut_v, sl_v, xt_v, da, ecol,
                 rya, ryb, ryc, ryd, rz1, rz2, ry2, agm, zrow, logit,
                 d1, d2, r1, r2, gram_d, gram_m, m1, m2,
                 sya, vya, syb, vyb, syc, vyc, syd, vyd, sz1, vz1, sz2, vz2, sy2, vy2, sam, vam,
                 w_sem, x_sem, sd, vd, sx, vx, sgd, vgd, sgm, vgm, o_sem):
    me = lax.axis_index('model')
    dat = lax.axis_index('data')
    z, y = lax.div(me, ny), lax.rem(me, ny)
    x, core = lax.div(dat, CORES), lax.rem(dat, CORES)
    n_model, nd = nz * ny, nx * CORES
    rows, n_dim = gg2.shape[2], gg2.shape[3]
    n_tok, n_ffn = sl_v.shape
    n_task = gg2.shape[0] // CORES
    n_class = ht_ref.shape[0]
    half_rows = rows // 2
    c1 = rya.shape[4]
    blk = ny * rows

    def peer_y(t):
        return (z * ny + t, dat)

    def peer_z(t):
        return (t * ny + y, dat)

    def peer_m(t):
        return (t, dat)

    def peer_d(t):
        return (me, t)

    def peer_x(t):
        return (me, t * CORES + core)

    other = (me, x * CORES + 1 - core)

    def offset(i):
        step = lax.div(i + 1, 2)
        return nz // 2 + jnp.where(lax.rem(i, 2) == 1, -step, step)

    def block_rows(i):
        return pl.ds(pl.multiple_of(lax.rem(z + offset(i), nz) * blk, blk), blk)

    def load_x(i):
        at = block_rows(i)
        return pltpu.make_async_copy(x_hbm.at[at, :], xd.at[at, :], x_sem.at[i])

    load_w1 = pltpu.make_async_copy(w1_hbm, w1_v, w_sem.at[0])
    load_w2 = pltpu.make_async_copy(w2_hbm, w2_v, w_sem.at[1])
    load_w1.start()
    load_x(0).start()
    load_w2.start()

    def start_x(i, _):
        load_x(i).start()
        return 0
    lax.fori_loop(1, nz, start_x, 0)

    barrier = pltpu.get_barrier_semaphore()
    greeted = [peer_d(lax.rem(dat + k, nd)) for k in range(1, nd)]
    greeted += [peer_m(lax.rem(me + k, n_model)) for k in range(1, n_model)]
    for peer in greeted:
        pl.semaphore_signal(barrier, inc=1, device_id=peer, device_id_type=pl.DeviceIdType.MESH)

    def hs(half):
        return pl.ds(half * half_rows, half_rows)

    left, right = pl.ds(0, c1), pl.ds(c1, n_dim - c1)

    def slot(off):
        return 2 * (nz // 2 - off) - 1 if off < nz // 2 else 2 * (off - nz // 2)

    own = slot(0)

    def add_y1(first):
        def add(dest, half, off, buf):
            def body(k, _):
                gg2[first + k, dest, hs(half), left] += buf[k]
                return 0
            lax.fori_loop(0, buf.shape[0], body, 0)
        return add

    def add_z1(dest, half, off, buf):
        gg2[slot(off), y, hs(half), left] += buf[...]

    def add_z2(dest, half, off, buf):
        def body(k, _):
            gg2[slot(off), k, hs(half), right] += buf[k]
            return 0
        lax.fori_loop(0, ny, body, 0)

    def add_y2(dest, half, off, buf):
        gg2[own, dest, hs(half), right] += buf[...]

    def landing(buf):
        return lambda d, i: buf.at[d, i]

    rings = {
        'z1': Ring(nz, z, peer_z, lambda t, h, o: gg2.at[slot(o), y, hs(h), left], landing(rz1), sz1.at[0], vz1, add_z1),
        'z2': Ring(nz, z, peer_z, lambda t, h, o: gg2.at[slot(o), :, hs(h), right], landing(rz2), sz2.at[0], vz2, add_z2),
        'y2': Ring(ny, y, peer_y, lambda t, h, o: gg2.at[own, t, hs(h), right], landing(ry2), sy2.at[0], vy2, add_y2),
    }
    first = 0
    for name, recv, send_sem, recv_sem in (('ya', rya, sya, vya), ('yb', ryb, syb, vyb), ('yc', ryc, syc, vyc), ('yd', ryd, syd, vyd)):
        group = pl.ds(first, recv.shape[2])
        rings[name] = Ring(ny, y, peer_y, lambda t, h, o, group=group: gg2.at[group, t, hs(h), left],
                           landing(recv), send_sem.at[0], recv_sem, add_y1(first))
        first += recv.shape[2]

    scale = np.float32(np.sqrt(2.0 / np.pi))

    def block(i, _):
        load_x(i).wait()
        at = block_rows(i)
        pre = jnp.dot(xd[at, :], w1_v[...], preferred_element_type=F32)
        square = pre * pre
        th = jnp.tanh(scale * (pre + np.float32(0.044715) * (square * pre)))
        cdf = 0.5 * (1.0 + th)
        act = (pre * cdf).astype(BF16)
        sl_v[at, :] = cdf + 0.5 * pre * (1.0 - th * th) * (scale * (1.0 + np.float32(3 * 0.044715) * square))
        ut_v[:, at] = act.T
        part = jnp.dot(act, w2_v[...], preferred_element_type=F32)
        gg2[i] = part.reshape(ny, rows, n_dim)
        return 0

    load_w1.wait()
    load_w2.wait()
    block(0, 0)
    pl.semaphore_wait(barrier, len(greeted))
    rings['z2'].begin(0)
    lax.fori_loop(1, 3, block, 0)
    rings['ya'].begin(0)
    rings['z2'].begin(1)
    rings['ya'].begin(1)
    lax.fori_loop(3, nz, block, 0)

    def flip(i, _):
        at = pl.ds(pl.multiple_of(i * blk, blk), blk)
        xt_v[:, at] = xd[at, :].T
        return 0
    ht_v[...] = jnp.zeros_like(ht_v)
    for c in range(n_class):
        ht_v[4 * c:4 * c + n_task, :] = ht_ref[c].astype(F32)
        for t in range(n_task):
            hb[4 * c + t] = jnp.broadcast_to(ht_ref[c, t:t + 1, :].astype(F32), (8, n_dim))

    order = [
        ('z2', 0), ('ya', 0), ('z2', 1), ('z2', 2), ('ya', 1), ('z2', 3), ('ya', 2), ('yb', 0), ('z2', 4), ('z1', 0),
        ('yb', 1), ('z2', 5), ('yb', 2), ('z1', 1), ('yc', 0), ('z2', 6), ('yc', 1), ('z1', 2), ('yc', 2), ('z1', 3),
        ('z1', 4), ('yd', 0), ('yd', 1), ('y2', 0), ('y2', 1), ('yd', 2), ('z1', 5), ('z1', 6), ('y2', 2)]
    begins = {('ya', 0): 'yb', ('ya', 2): 'z1', ('yb', 0): 'yc', ('yc', 0): 'yd', ('z2', 6): 'y2'}
    for event in order:
        name, i = event
        rings[name].step(i)
        if event == ('z2', 2):
            lax.fori_loop(0, nz, flip, 0)
        if event in begins:
            rings[begins[event]].begin(0)
            rings[begins[event]].begin(1)

    mine = pl.ds(pl.multiple_of(me * rows, rows), rows)
    zrow[...] = (xd[mine, :].astype(F32) + gg2[own, y]).astype(BF16)
    logit[...] = lax.dot_general(ht_v[...].astype(BF16), zrow[...], (((1,), (1,)), ((), ())), preferred_element_type=F32)
    per = 128 // rows
    wide = lab_ref[:, pl.ds(pl.multiple_of(lax.div(me, per) * 128, 128), 128)]
    lab = wide[:, :rows]
    for k in range(1, per):
        lab = jnp.where(lax.rem(me, per) == k, wide[:, k * rows:(k + 1) * rows], lab)
    agm[me] = jnp.zeros((8, 128), F32)
    for t in range(n_task):
        ls = [logit[4 * c + t:4 * c + t + 1, :] for c in range(n_class)]
        top = functools.reduce(jnp.maximum, ls)
        es = [jnp.exp(v - top) for v in ls]
        total = functools.reduce(jnp.add, es)
        for c in range(n_class):
            row, first = 2 * c + t // 2, t % 2 * rows
            agm[me, row:row + 1, first:first + rows] = (
                es[c] / total - jnp.where(lab[t:t + 1, :] == c, 1.0, 0.0)) / n_total

    def exchange(n, pos, peer, buf, send_sem, recv_sem, use):
        def copy(k, src):
            return pltpu.make_async_remote_copy(
                src_ref=buf.at[pos], dst_ref=buf.at[src], send_sem=send_sem.at[0], recv_sem=recv_sem.at[k],
                device_id=peer(lax.rem(pos + k, n)), device_id_type=pl.DeviceIdType.MESH)
        for k in range(1, n):
            copy(k, pos).start()
        use(pos)
        for k in range(1, n):
            src = lax.rem(pos + n - k, n)
            copy(k, src).wait_recv()
            use(src)

    def turn(k):
        ecol[k] = agm[k].T

    exchange(n_model, me, peer_m, agm, sam, vam, turn)
    for buf, send_sem, recv_sem in ((rya, sya, vya), (ryb, syb, vyb), (ryc, syc, vyc), (ryd, syd, vyd),
                                    (rz1, sz1, vz1), (rz2, sz2, vz2), (ry2, sy2, vy2)):
        sent(buf, send_sem.at[0], recv_sem.at[0, 0], other)

    def make_dz(t, cols):
        def body(i, _):
            at = pl.ds(pl.multiple_of(i * rows, rows), rows)
            first = t % 2 * rows
            es = [jnp.broadcast_to(ecol[i, first:first + rows, 2 * c + t // 2:2 * c + t // 2 + 1], (rows, 128))
                  for c in range(n_class)]
            for j in range(cols[0], cols[1], 128):
                parts = [es[c] * jnp.concatenate([hb[4 * c + t, :, j:j + 128]] * (rows // 8), axis=0)
                         for c in range(n_class)]
                xd[at, j:j + 128] = functools.reduce(jnp.add, parts).astype(BF16)
            return 0
        lax.fori_loop(0, n_model, body, 0, unroll=4)

    tile = 256
    q1 = gg1.shape[2]

    def make_g2(t, cols):
        def body(i, _):
            at = pl.ds(pl.multiple_of(i * tile, tile), tile)
            out = jnp.dot(ut_v[...], xd[:, at], preferred_element_type=F32).reshape(nx, CORES, rows, tile)
            for c in range(CORES):
                gg2[CORES * t + c, :, :, at] = out[:, c]
            return 0
        lax.fori_loop(cols[0] // tile, cols[1] // tile, body, 0)

    def make_da(part):
        def body(i, _):
            at = pl.ds(pl.multiple_of(i * 2 * tile, 2 * tile), 2 * tile)
            out = lax.dot_general(xd[at, :], w2_v[...], (((1,), (1,)), ((), ())), preferred_element_type=F32)
            da[at, :] = (out * sl_v[at, :]).astype(BF16)
            return 0
        n_half = n_tok // (4 * tile)
        lax.fori_loop(part * n_half, (part + 1) * n_half, body, 0)

    def make_g1(t, cols):
        hx = nx // 2

        def body(i, _):
            at = pl.ds(pl.multiple_of(i * tile, tile), tile)
            for k in (0, 1):
                part = pl.ds(k * (n_dim // 2), n_dim // 2)
                out = jnp.dot(xt_v[part, :], da[:, at], preferred_element_type=F32).reshape(hx, CORES, q1, tile)
                for c in range(CORES):
                    gg1[CORES * t + c, k * hx:(k + 1) * hx, :, at] = out[:, c]
            return 0
        lax.fori_loop(cols[0] // tile, cols[1] // tile, body, 0)

    all1, all2 = (0, n_ffn), (0, n_dim)
    stages = [(2, 0, (0, n_dim // 2)), (2, 0, (n_dim // 2, n_dim)),
              (1, 0, (0, n_ffn // 2)), (1, 0, (n_ffn // 2, n_ffn))]
    for t in range(1, n_task):
        stages += [(2, t, all2), (1, t, all1)]
    n_stage = len(stages)
    sets = {2: (gg2, d2, r2), 1: (gg1, d1, r1)}

    def columns(s):
        first, last = stages[s][2]
        return pl.ds(first, last - first)

    def swap(s):
        g, buf, _ = sets[stages[s][0]]
        t = stages[s][1]
        return pltpu.make_async_remote_copy(
            src_ref=g.at[CORES * t + 1 - core, :, :, columns(s)], dst_ref=buf.at[t, :, :, columns(s)],
            send_sem=sd.at[stages[s][0] - 1], recv_sem=vd.at[s], device_id=other, device_id_type=pl.DeviceIdType.MESH)

    def ring_of(s):
        g, _, r = sets[stages[s][0]]
        t = stages[s][1]
        half = g.shape[2] // 2

        def chunk(dest, h, off):
            return g.at[CORES * t + core, dest, pl.ds(h * half, half), columns(s)]

        def add(dest, h, off, buf):
            g[CORES * t + core, dest, pl.ds(h * half, half), columns(s)] += buf[...]

        def into(d, i):
            return r.at[t, d, i, :, columns(s)]

        return Ring(nx, x, peer_x, chunk, into, sx.at[stages[s][0] - 1], vx.at[s], add)

    def launch(s):
        g, buf, _ = sets[stages[s][0]]
        t = stages[s][1]
        swap(s).wait_recv()

        def body(k, _):
            g[CORES * t + core, k, :, columns(s)] += buf[t, k, :, columns(s)]
            return 0
        lax.fori_loop(0, nx, body, 0)
        if s >= 6:
            ring_of(s - 2).step(0)
        ring_of(s).begin(0)
        ring_of(s).begin(1)

    for s in range(n_stage):
        which, t, cols = stages[s]
        if which == 2:
            make_dz(t, cols)
            if s == 1 or s >= 4:
                launch(s - 1)
            make_g2(t, cols)
        elif s == 3:
            make_g1(t, cols)
        else:
            make_da(0)
            launch(s - 1)
            make_da(1)
            if s == 2:
                ring_of(0).step(0)
            make_g1(t, cols)
        swap(s).start()
        if s == 2:
            ring_of(1).step(0)
        if s == 3:
            launch(2)
        if s == 4:
            ring_of(2).step(0)
            ring_of(3).step(0)
    launch(n_stage - 1)
    for s in (n_stage - 2, n_stage - 1):
        ring_of(s).step(0)
    def settle(s):
        ring_of(s).step(1)
        ring_of(s).step(2)

    for s in range(n_stage - 1):
        settle(s)

    pairs = [(i, j) for i in range(n_task) for j in range(i, n_task)]

    def fold(g, accs):
        width = g.shape[3]

        def body(k, accs):
            at = pl.ds(pl.multiple_of(k * 8, 8), 8)
            vals = [g[CORES * t + core, x, at, :] for t in range(n_task)]
            return tuple(acc + sum((vals[i] * vals[j])[:, w:w + 128] for w in range(0, width, 128))
                         for acc, (i, j) in zip(accs, pairs))
        return lax.fori_loop(0, g.shape[2] // 8, body, accs)

    accs = tuple(jnp.zeros((8, 128), F32) for _ in pairs)
    accs = fold(gg2, accs)
    settle(n_stage - 1)
    accs = fold(gg1, accs)
    lane = lax.broadcasted_iota(jnp.int32, (1, 128), 1)
    part = jnp.zeros((1, 128), F32)
    for acc, (i, j) in zip(accs, pairs):
        hit = (lane == n_task * i + j) | (lane == n_task * j + i)
        part = jnp.where(hit, jnp.sum(jnp.sum(acc, axis=0, keepdims=True), axis=1, keepdims=True), part)

    def all_sum(n, pos, peer, buf, send_sem, recv_sem, val):
        buf[pos, 0:1, :] = val
        for k in range(1, n):
            pltpu.make_async_remote_copy(
                src_ref=buf.at[pos, pl.ds(0, 1), :], dst_ref=buf.at[pos, pl.ds(0, 1), :],
                send_sem=send_sem.at[0], recv_sem=recv_sem.at[0],
                device_id=peer(lax.rem(pos + k, n)), device_id_type=pl.DeviceIdType.MESH).start()
        rest = buf.at[pl.ds(0, n - 1), pl.ds(0, 1), :]
        pltpu.make_async_remote_copy(
            src_ref=rest, dst_ref=rest, send_sem=send_sem.at[0], recv_sem=recv_sem.at[0],
            device_id=other, device_id_type=pl.DeviceIdType.MESH).wait_recv()
        out = buf[0, 0:1, :]
        for k in range(1, n):
            out = out + buf[k, 0:1, :]
        return out

    part = all_sum(nd, dat, peer_d, gram_d, sgd, vgd, part)
    part = all_sum(n_model, me, peer_m, gram_m, sgm, vgm, part)

    gram = [[jnp.broadcast_to(part[:, n_task * i + j:n_task * i + j + 1], (1, 128)) for j in range(n_task)]
            for i in range(n_task)]
    trace_scale = functools.reduce(jnp.add, [gram[i][i] for i in range(n_task)]) / n_task

    def eg(i, ws):
        ups = []
        for t in range(n_task):
            prod = functools.reduce(jnp.add, [gram[t][j] * ws[j] for j in range(n_task)])
            ups.append(ws[t] * jnp.exp(-prod / trace_scale))
        total = functools.reduce(jnp.add, ups)
        return tuple(up / total for up in ups)

    ws = tuple(jnp.full((1, 128), 1.0 / n_task, F32) for _ in range(n_task))
    ws = lax.fori_loop(0, STEPS, eg, ws)
    weights = jnp.zeros((1, 128), F32)
    for t in range(n_task):
        weights = jnp.where(lane == t, ws[t], weights)
    a_out[0:1, :] = weights
    writes = []

    def mix(g, out):
        width = g.shape[3]

        def body(k, _):
            at = pl.ds(pl.multiple_of(k * 8, 8), 8)
            for w in range(0, width, 128):
                acc = ws[0] * g[core, x, at, w:w + 128]
                for t in range(1, n_task):
                    acc = acc + ws[t] * g[CORES * t + core, x, at, w:w + 128]
                out[at, w:w + 128] = acc
            return 0
        lax.fori_loop(0, g.shape[2] // 8, body, 0)
    for k, (g, stage_out, out) in enumerate(((gg1, m1, g1_out), (gg2, m2, g2_out))):
        mix(g, stage_out)
        writes.append(pltpu.make_async_copy(stage_out, out, o_sem.at[k]))
        writes[-1].start()

    for c in writes:
        c.wait()
    sent(agm.at[pl.ds(0, n_model - 1)], sam.at[0], vam.at[0], other)
    sent(gram_d.at[pl.ds(0, nd - 1), pl.ds(0, 1), :], sgd.at[0], vgd.at[0], other)
    sent(gram_m.at[pl.ds(0, n_model - 1), pl.ds(0, 1), :], sgm.at[0], vgm.at[0], other)
    for k, (d, r) in enumerate(((d1, r1), (d2, r2))):
        sent(d, sd.at[k], vd.at[0], other)
        sent(r, sx.at[k], vx.at[0, 0, 0], other)


def write_kernel(a_ref, g1_ref, g2_ref, a_out, g1_out, g2_out):
    a_out[...] = a_ref[0:1, 0:a_out.shape[1]]
    g1_out[...] = g1_ref[...]
    g2_out[...] = g2_ref[...]


def solution(mesh, ny=NY):
    n_data = mesh.shape['data']
    n_model = mesh.shape['model']
    nz = n_model // ny
    nx = n_data // CORES

    def local_step(tokens, w_up, w_down, task_heads, labels):
        n_tok, n_dim = tokens.shape
        n_ffn = w_up.shape[1]
        n_task, _, n_class = task_heads.shape
        rows = n_tok // n_model
        hr = rows // 2
        c1 = 5 * n_dim // 8
        c2 = n_dim - c1
        f1 = n_dim // n_data
        f2 = n_ffn // n_data
        heads = jnp.transpose(task_heads, (2, 0, 1))
        vm = pl.BlockSpec(memory_space=pltpu.VMEM)
        hbm = pl.BlockSpec(memory_space=pl.ANY)
        dma = pltpu.SemaphoreType.DMA
        outs = [jax.ShapeDtypeStruct((f1, n_ffn), F32), jax.ShapeDtypeStruct((f2, n_dim), F32)]
        stages = 2 * n_task + 2

        results = pl.pallas_call(
            functools.partial(trunk_kernel, nz, ny, nx, n_tok * n_data),
            out_shape=[jax.ShapeDtypeStruct((8, 128), F32)] + outs,
            in_specs=[hbm] * 3 + [vm] * 2, out_specs=[vm, hbm, hbm],
            scratch_shapes=[
                pltpu.VMEM((n_tok, n_dim), BF16), pltpu.VMEM((n_dim, n_ffn), BF16), pltpu.VMEM((n_ffn, n_dim), BF16),
                pltpu.VMEM((16, n_dim), F32), pltpu.VMEM((n_class * n_task, 8, n_dim), F32),
                pltpu.VMEM((CORES * n_task, nx, f2, n_dim), F32), pltpu.VMEM((CORES * n_task, nx, f1, n_ffn), F32),
                pltpu.VMEM((n_ffn, n_tok), BF16), pltpu.VMEM((n_tok, n_ffn), F32), pltpu.VMEM((n_dim, n_tok), BF16),
                pltpu.VMEM((n_tok, n_ffn), BF16), pltpu.VMEM((n_model, 128, 8), F32),
                pltpu.VMEM((2, ny - 1, 3, hr, c1), F32), pltpu.VMEM((2, ny - 1, nz - 6, hr, c1), F32),
                pltpu.VMEM((2, ny - 1, 2, hr, c1), F32), pltpu.VMEM((2, ny - 1, 1, hr, c1), F32),
                pltpu.VMEM((2, nz - 1, hr, c1), F32),
                pltpu.VMEM((2, nz - 1, ny, hr, c2), F32), pltpu.VMEM((2, ny - 1, hr, c2), F32),
                pltpu.VMEM((n_model, 8, 128), F32),
                pltpu.VMEM((rows, n_dim), BF16), pltpu.VMEM((16, rows), F32),
                pltpu.VMEM((n_task, nx, f1, n_ffn), F32), pltpu.VMEM((n_task, nx, f2, n_dim), F32),
                pltpu.VMEM((n_task, 2, nx - 1, f1 // 2, n_ffn), F32), pltpu.VMEM((n_task, 2, nx - 1, f2 // 2, n_dim), F32),
                pltpu.VMEM((n_data, 8, 128), F32), pltpu.VMEM((n_model, 8, 128), F32),
                pltpu.VMEM((f1, n_ffn), F32), pltpu.VMEM((f2, n_dim), F32),
                *[dma((1,)), dma((2, ny - 1))] * 4, dma((1,)), dma((2, nz - 1)),
                dma((1,)), dma((2, nz - 1)), dma((1,)), dma((2, ny - 1)),
                dma((1,)), dma((n_model,)),
                dma((2,)), dma((nz,)), dma((2,)), dma((stages,)), dma((2,)), dma((stages, 2, nx - 1)),
                dma((1,)), dma((1,)), dma((1,)), dma((1,)), dma((2,))],
            compiler_params=pltpu.CompilerParams(collective_id=0, has_side_effects=True, vmem_limit_bytes=VMEM_LIMIT),
            name='trunk',
        )(tokens, w_up, w_down, heads, labels)
        weights, g1, g2 = pl.pallas_call(
            write_kernel, out_shape=[jax.ShapeDtypeStruct((1, n_task), F32)] + outs,
            in_specs=[vm] * 3, out_specs=[vm] * 3, name='write',
        )(*results)
        return weights.reshape(n_task), g1, g2

    return jax.shard_map(
        local_step, mesh=mesh,
        in_specs=(P('data', None), P(None, 'model'), P('model', None), P(None, None, None), P(None, 'data')),
        out_specs=(P(None), P('data', 'model'), P(('model', 'data'), None)),
        check_vma=False)
```
